128 devices in a mesh: ops: 32 (over z, y, core), site: 4 (over x).
Axes of the slice: x: 4, y: 4, z: 4, core: 2. Of those that a mesh axis runs over, the one named last changes fastest.
Arguments:
- wavefunction: bfloat16 [2048, 2048], replicated, may hold values from -6 to 6
- left_blocks: bfloat16 [256, 16, 192, 192], P('ops', 'site'), may hold values from -0.4375 to 0.4375
- right_blocks: bfloat16 [256, 16, 192, 192], P('ops', 'site'), may hold values from -0.078125 to 0.078125
- left_sector: int32 [2048], replicated, may hold values from 0 to 15, as said below
- right_sector: int32 [2048], replicated, may hold values from 0 to 15, as said below
- term_count: int32 [32], P('ops'), may hold values from 1 to 8, as said below
- left_energy: float32 [2048], replicated, may hold values from -1 to 1
- right_energy: float32 [2048], replicated, may hold values from -1 to 1
- subspace: bfloat16 [2, 16, 192, 2048], P(None, 'site'), may hold values from -0.0078125 to 0.0078125
Outputs:
- sigma: bfloat16 [16, 192, 2048], P('site')
- projections: float32 [2], replicated
The draws below stay inside these ranges and needn't reach their ends.
Inputs may be any that keep to these rules, and one draw needn't show every extreme that they name: `left_sector`: sector ids never fall along the bond; each of the 16 sectors has 1 to 192 states and one has exactly 192. `right_sector`: sector ids never fall along the bond; each of the 16 sectors has 1 to 192 states and one has exactly 192. `term_count`: some group has all 8 slots live.
All inputs are finite; a program needn't handle non-finite values.
Results may differ from the reference program's by a relative error of at most 0.0045.
Values may be sent and summed in bfloat16 or wider, within the bound.
A program may use at most 192 MiB of HBM per device.

```python
import jax
import jax.numpy as jnp
from jax import lax

M = 2048
NB = 16
MAXB = 192
TERMS_DEV = 8
SUB = 2
TERMS = 256
N_OPS = 32


def draw_term_count(key, part):
    base_counts = jax.random.randint(jax.random.fold_in(key, 11), (N_OPS,), 1, TERMS_DEV // 2 + 1)
    fullest = jax.random.randint(jax.random.fold_in(key, 12), (), 0, N_OPS)
    return jnp.where(jnp.arange(N_OPS) == fullest, TERMS_DEV, base_counts).astype(jnp.int32)


def sector_draw(key):
    biggest = jax.random.randint(jax.random.fold_in(key, 1), (), 0, NB)
    remaining = jnp.int32(M - MAXB)
    sizes = []
    for label in range(NB):
        after = jnp.int32(NB - 1 - label) - (biggest > label).astype(jnp.int32)
        lower = jnp.maximum(1, remaining - after * MAXB)
        upper = jnp.minimum(MAXB, remaining - after)
        picked = jax.random.randint(jax.random.fold_in(key, 100 + label), (), lower, upper + 1)
        is_big = biggest == label
        size_now = jnp.where(is_big, jnp.int32(MAXB), picked).astype(jnp.int32)
        remaining = jnp.where(is_big, remaining, remaining - picked).astype(jnp.int32)
        sizes.append(size_now)
    ends = jnp.cumsum(jnp.stack(sizes)).astype(jnp.int32)
    positions = jnp.arange(M, dtype=jnp.int32)
    return jnp.sum((ends[None, :] <= positions[:, None]).astype(jnp.int32), axis=1).astype(jnp.int32)


def draw_left_sector(key, part):
    return sector_draw(jax.random.fold_in(key, 31))


def draw_right_sector(key, part):
    return sector_draw(jax.random.fold_in(key, 32))


def shard_levels(own_key, shape, shards, low, top_value):
    def one(axis_at, parts):
        heights = jax.random.uniform(jax.random.fold_in(jax.random.fold_in(own_key, 6), axis_at), (parts,), jnp.float32, low / len(shards), top_value / len(shards))
        return jnp.repeat(jnp.exp(heights), shape[axis_at] // parts).reshape((-1,) + (1,) * (len(shape) - axis_at - 1))

    loudness = one(*shards[0])
    for cut in shards[1:]:
        loudness = loudness * one(*cut)
    return loudness


def scatter_about(key, shape, deviation, reach, shards=(), held_as=jnp.bfloat16):
    drawn = deviation * jax.random.normal(key, shape, jnp.float32)
    if shards:
        drawn = drawn * shard_levels(key, shape, shards, -0.22, 0.18)
    return jnp.clip(drawn, -reach, reach).astype(held_as)


def setup_inputs(seed: int = 0) -> dict:
    seeds = jax.random.split(jax.random.key(seed), 10)
    wavefunction = scatter_about(seeds[0], (M, M), 1.0, 6.0)
    left_blocks = scatter_about(seeds[1], (TERMS, NB, MAXB, MAXB), MAXB ** -0.5, 0.4375, ((0, 32), (1, 4)))
    right_blocks = scatter_about(seeds[2], (TERMS, NB, MAXB, MAXB), (MAXB * TERMS_DEV * N_OPS // 8) ** -0.5, 0.078125, ((0, 32), (1, 4)))
    left_sector = draw_left_sector(jax.random.fold_in(seeds[9], 71), 0)
    right_sector = draw_right_sector(jax.random.fold_in(seeds[9], 71), 0)
    term_count = draw_term_count(jax.random.fold_in(seeds[9], 71), 0)
    left_energy = jnp.clip(jax.random.uniform(seeds[6], (M,), jnp.float32, -1.0, 1.0), -1.0, 1.0)
    right_energy = jnp.clip(jax.random.uniform(seeds[7], (M,), jnp.float32, -1.0, 1.0), -1.0, 1.0)
    subspace = scatter_about(seeds[8], (SUB, NB, MAXB, M), (1.0 / M), 0.0078125, ((1, 4),))
    return {"wavefunction": wavefunction, "left_blocks": left_blocks, "right_blocks": right_blocks, "left_sector": left_sector, "right_sector": right_sector, "term_count": term_count, "left_energy": left_energy, "right_energy": right_energy, "subspace": subspace}


def sector_tables(sector_ids, sectors):
    labels = jnp.arange(sectors, dtype=jnp.int32)
    sector_starts = jnp.sum((sector_ids[None, :] < labels[:, None]).astype(jnp.int32), axis=1)
    sector_sizes = jnp.sum((sector_ids[None, :] == labels[:, None]).astype(jnp.int32), axis=1)
    return sector_starts.astype(jnp.int32), sector_sizes.astype(jnp.int32)


def reference(wavefunction, left_blocks, right_blocks, left_sector, right_sector, term_count, left_energy, right_energy, subspace):
    left_start, left_size = sector_tables(left_sector, NB)
    right_start, right_size = sector_tables(right_sector, NB)
    positions = jnp.arange(MAXB, dtype=jnp.int32)
    left_inside = positions[None, :] < left_size[:, None]
    right_inside = positions[None, :] < right_size[:, None]
    left_masks = left_inside[:, :, None] & left_inside[:, None, :]
    right_masks = right_inside[:, :, None] & right_inside[:, None, :]
    psi_padded = jnp.concatenate([wavefunction, jnp.zeros((MAXB, M), wavefunction.dtype)], axis=0)
    psi_slabs = jax.vmap(lambda row_start: lax.dynamic_slice_in_dim(psi_padded, row_start, MAXB, 0))(left_start)
    slab_values = psi_slabs.astype(jnp.float32)
    row_count = NB * MAXB

    def term_product(accum, term_idx):
        live = (term_idx % TERMS_DEV) < term_count[term_idx // TERMS_DEV]

        def apply_term(summed_in):
            blocks = jnp.where(left_masks, left_blocks[term_idx], jnp.zeros((), left_blocks.dtype)).astype(jnp.float32)
            left_image = jnp.einsum("qab,qbc->qac", blocks, slab_values, precision=lax.Precision.HIGHEST)
            rounded = lax.optimization_barrier(left_image.astype(jnp.bfloat16)).astype(jnp.float32)
            rounded = rounded.reshape(row_count, M)
            padded_image = jnp.concatenate([rounded, jnp.zeros((row_count, MAXB), jnp.float32)], axis=1)
            right_terms = jnp.where(right_masks, right_blocks[term_idx], jnp.zeros((), right_blocks.dtype)).astype(jnp.float32)

            def one_sector(sector, summed):
                col_start = right_start[sector]
                window = lax.dynamic_slice_in_dim(padded_image, col_start, MAXB, 1)
                added = jnp.dot(window, right_terms[sector].T, precision=lax.Precision.HIGHEST)
                previous = lax.dynamic_slice_in_dim(summed, col_start, MAXB, 1)
                return lax.dynamic_update_slice_in_dim(summed, previous + added, col_start, 1)

            return lax.fori_loop(0, NB, one_sector, summed_in)

        return lax.cond(live, apply_term, lambda kept: kept, accum), None

    terms_padded, ignored = lax.scan(term_product, jnp.zeros((row_count, M + MAXB), jnp.float32), jnp.arange(TERMS_DEV * N_OPS, dtype=jnp.int32))
    terms = terms_padded[:, :M].reshape(NB, MAXB, M)
    psi_rows = jnp.where(left_inside[:, :, None], slab_values, jnp.float32(0.0))
    energy_padded = jnp.concatenate([left_energy, jnp.zeros((MAXB,), jnp.float32)])
    energy_rows = jax.vmap(lambda row_start: lax.dynamic_slice_in_dim(energy_padded, row_start, MAXB, 0))(left_start)
    sigma_full = terms + (energy_rows[:, :, None] + right_energy[None, None, :]) * psi_rows
    projections = jnp.sum(subspace.astype(jnp.float32) * sigma_full[None], axis=(1, 2, 3))
    return sigma_full.astype(jnp.bfloat16), projections
```

```python
import jax
import jax.numpy as jnp
from jax import lax
from jax.experimental import pallas as pl
from jax.experimental.pallas import tpu as pltpu
from jax.sharding import PartitionSpec as P

W = 192
SLOTS = 8
NS = 2
NC = SLOTS // NS
BOND = 2048
BF = jnp.bfloat16
F32 = jnp.float32
MESH = pl.DeviceIdType.MESH


def iota(shape, dim):
    return lax.broadcasted_iota(jnp.int32, shape, dim)


def one_hot(mask):
    return jnp.where(mask, F32(1), F32(0)).astype(BF)


def packed_index(pos, parity):
    tail = pos - 64 * parity
    idx = jnp.where(pos < 128, pos, tail)
    ok = (pos < 128) | ((tail >= 128) & (tail < W))
    return idx, ok


def piece_offsets(bits):
    offs = []
    for qi in range(4):
        off = [0]
        for s in range(4):
            off.append(off[-1] + bits[(qi + s) % 4] * (384 >> s))
        offs.append(off)
    return offs


def label_bits(y, z):
    return (((y + 1) // 2) % 2, ((z + 1) // 2) % 2, y // 2, z // 2)


def prep_body(
    lstart, lsize, rstart, rsize, psi_v, lenergy, renergy, sub_hbm,
    pp_hbm, diag, subp, gath, pp, stack, sub_sem, pp_sem,
):
    x = lax.axis_index("site")
    o = lax.axis_index("ops")
    c = o % 2
    x_l = x + 1 - 2 * (x % 2)
    x_r = 3 - x
    offs = piece_offsets(label_bits((o // 2) % 4, o // 8))

    def sub_copy(qi, k):
        off = offs[qi][4]
        return pltpu.make_async_copy(
            sub_hbm.at[k, off // W, pl.ds(pl.multiple_of(off % W, 16), 48), :],
            stack.at[qi, pl.ds(48 + 48 * k, 48), :], sub_sem.at[qi, k])

    for qi in range(4):
        for k in range(2):
            sub_copy(qi, k).start()

    def row_hot(q, first, rows, packed):
        rs = lstart[q]
        base = pl.multiple_of(jnp.minimum((rs // 16) * 16, BOND - 256), 16)
        pos = iota((rows, 256), 0) + first
        if packed:
            idx, ok = packed_index(pos, q % 2)
        else:
            idx, ok = pos, pos < W
        ok = ok & (idx < lsize[q])
        return base, one_hot(ok & (iota((rows, 256), 1) == idx + (rs - base)))

    def rows_of(i, carry):
        q = jnp.where(i < 4, x * 4 + i, x_l * 4 + i - 4)
        base, hot = row_hot(q, 0, 256, True)
        for n in range(4):
            win = psi_v[pl.ds(base, 256), pl.ds(n * 512, 512)]
            gath[pl.ds(pl.multiple_of(i * 256, 256), 256), pl.ds(n * 512, 512)] = jnp.dot(
                hot, win, preferred_element_type=F32).astype(BF)
        return carry

    lax.fori_loop(0, 8, rows_of, 0)

    def pp_copy(j):
        return pltpu.make_async_copy(pp.at[j], pp_hbm.at[j], pp_sem.at[j])

    def cols_of(j, carry):
        q = jnp.where(j < 4, x * 4 + j, x_r * 4 + j - 4)
        cs = rstart[q]
        cb = pl.multiple_of(jnp.minimum((cs // 128) * 128, BOND - 384), 128)
        idx, ok = packed_index(iota((384, 256), 1), q % 2)
        ok = ok & (idx < rsize[q])
        hot = one_hot(ok & (iota((384, 256), 0) == idx + (cs - cb)))
        for m in range(4):
            win = gath[pl.ds(m * 512, 512), pl.ds(cb, 384)]
            pp[j, pl.ds(m * 512, 512), :] = jnp.dot(win, hot, preferred_element_type=F32).astype(BF)
        pp_copy(j).start()
        return carry

    lax.fori_loop(0, 8, cols_of, 0)

    re = renergy[...]
    hi = re.astype(BF)
    rem = re - hi.astype(F32)
    mid = rem.astype(BF)
    low = (rem - mid.astype(F32)).astype(BF)
    rows16 = iota((16, BOND), 0)
    er3 = jnp.where(rows16 == 0, hi.astype(F32),
                    jnp.where(rows16 == 1, mid.astype(F32),
                              jnp.where(rows16 == 2, low.astype(F32), F32(0)))).astype(BF)
    for qi in range(4):
        l2, t = qi // 2, qi % 2
        off = offs[qi][4]
        q = x * 4 + off // W
        a0 = off % W
        base, hot = row_hot(q, a0, 48, False)
        for n in range(4):
            win = psi_v[pl.ds(base, 256), pl.ds(n * 512, 512)]
            stack[qi, pl.ds(0, 48), pl.ds(n * 512, 512)] = jnp.dot(
                hot, win, preferred_element_type=F32).astype(BF)
        stack[qi, pl.ds(144, 16), :] = er3
        for k in range(2):
            sub_copy(qi, k).wait()
        xt = x if t == 0 else x_l
        site = xt + c * (3 - 2 * xt)
        total = None
        for par in range(2):
            qr = site * 4 + 2 * l2 + par
            cs = rstart[qr]
            cb = pl.multiple_of(jnp.minimum((cs // 128) * 128, BOND - 384), 128)
            j = iota((384, 384), 1) - W * par
            hot2 = one_hot((j >= 0) & (j < W) & (j < rsize[qr]) & (iota((384, 384), 0) == j + (cs - cb)))
            part = jnp.dot(stack[qi, :, pl.ds(cb, 384)], hot2, preferred_element_type=F32)
            total = part if total is None else total + part
        lb = pl.multiple_of(jnp.minimum((lstart[q] // 128) * 128, BOND - 384), 128)
        shift = lstart[q] - lb + a0
        pick = iota((48, 384), 1) == iota((48, 384), 0) + shift
        el = jnp.sum(jnp.where(pick, lenergy[:, pl.ds(lb, 384)], F32(0)), axis=1, keepdims=True)
        er = total[144:145] + total[145:146] + total[146:147]
        diag[qi] = (el + er) * total[:48]
        subp[qi, 0] = total[48:96]
        subp[qi, 1] = total[96:144]

    for j in range(8):
        pp_copy(j).wait()


def body(
    lsize, count, pp_hbm, left_hbm, right_hbm, diag, subp,
    out_hbm, proj_out,
    slabs_v, pp, raw, lown, lfor, rown, rfor, li, acc,
    drecv, rs0, rs1, rs2, rs3, xrecv, pvs, pvr,
    raw_sem, pp_sem, out_sem,
    l_ss, l_rs, r_ss, r_rs, d_ss, d_rs, rs_ss, rs_rs, x_ss, x_rs,
    ag_ss, ag_rs, fw_ss, fw_rs, pv_ss, pv_rs,
):
    x = lax.axis_index("site")
    o = lax.axis_index("ops")
    c = o % 2
    y = (o // 2) % 4
    z = o // 8
    x_l = x + 1 - 2 * (x % 2)
    x_r = 3 - x
    to_l = {"site": x_l}
    to_r = {"site": x_r}
    sib = {"ops": o + 1 - 2 * c}
    y_a = y + 1 - 2 * (y % 2)
    z_a = z + 1 - 2 * (z % 2)
    dims = (
        {"ops": o + 2 * (y_a - y)},
        {"ops": o + 8 * (z_a - z)},
        {"ops": o + 2 * (3 - 2 * y)},
        {"ops": o + 8 * (3 - 2 * z)},
    )
    bits = label_bits(y, z)

    def raw_copies(ch):
        buf = ch % 2
        return (
            pltpu.make_async_copy(left_hbm.at[pl.ds(NS * ch, NS)], raw.at[buf, 0], raw_sem.at[buf, 0]),
            pltpu.make_async_copy(right_hbm.at[pl.ds(NS * ch, NS)], raw.at[buf, 1], raw_sem.at[buf, 1]),
        )

    for ch in range(2):
        for cp in raw_copies(ch):
            cp.start()
    pp_copy = pltpu.make_async_copy(pp_hbm, pp, pp_sem)
    pp_copy.start()
    offs = piece_offsets(bits)

    barrier = pltpu.get_barrier_semaphore()
    for who in (to_l, to_r, sib, *dims):
        pl.semaphore_signal(barrier, inc=1, device_id=who, device_id_type=MESH)

    zrow = jnp.zeros((NC, NS, 2, 3, 64, 128), BF)
    for buf in (rown, rfor):
        for start in (0, 256):
            buf[:, :, :, :, pl.ds(start, 64), :] = zrow

    def l_copy(ch):
        return pltpu.make_async_remote_copy(
            src_ref=lown.at[ch], dst_ref=lfor.at[ch], send_sem=l_ss.at[ch], recv_sem=l_rs.at[ch],
            device_id=to_l, device_id_type=MESH)

    def r_copy(ch):
        rows = pl.ds(64, W)
        return pltpu.make_async_remote_copy(
            src_ref=rown.at[ch, :, :, :, rows, :], dst_ref=rfor.at[ch, :, :, :, rows, :],
            send_sem=r_ss.at[ch], recv_sem=r_rs.at[ch], device_id=to_r, device_id_type=MESH)

    def pack(ch):
        buf = ch % 2

        def one(k, carry):
            s = k // 2
            p = k % 2
            row = iota((W, 128), 0)
            live = NS * ch + s < count[0]
            keep = []
            for par in range(2):
                size = jnp.where(live, lsize[x * 4 + 2 * p + par], 0)
                keep.append(one_hot(row < size))
            ev = raw[buf, 0, s, 2 * p]
            od = raw[buf, 0, s, 2 * p + 1]
            lown[ch, s, p, 0] = ev[:, :128] * keep[0]
            lown[ch, s, p, 1] = od[:, :128] * keep[1]
            lown[ch, s, p, 2] = jnp.concatenate(
                [ev[:, 128:] * keep[0][:, :64], od[:, 128:] * keep[1][:, :64]], axis=1)
            ev = raw[buf, 1, s, 2 * p]
            od = raw[buf, 1, s, 2 * p + 1]
            rows = pl.ds(64, W)
            rown[ch, s, p, 0, rows, :] = ev[:, :128]
            rown[ch, s, p, 1, rows, :] = od[:, :128]
            rown[ch, s, p, 2, rows, :] = jnp.concatenate([ev[:, 128:], od[:, 128:]], axis=1)
            return carry

        lax.fori_loop(0, 2 * NS, one, 0)

    for ch in range(NC):
        for cp in raw_copies(ch):
            cp.wait()
        pack(ch)
        if ch == 0:
            pl.semaphore_wait(barrier, 7)
        if ch + 2 < NC:
            for cp in raw_copies(ch + 2):
                cp.start()
        l_copy(ch).start()
        r_copy(ch).start()

    pp_copy.wait()

    def clear(r, carry):
        for a in range(2):
            for b in range(2):
                acc[a, b, pl.ds(pl.multiple_of(r * 192, 192), 192), :] = jnp.zeros((192, 384), F32)
        return carry

    lax.fori_loop(0, 8, clear, 0)

    def rectangle(ch, lsrc, rsrc, h, g):
        def pair(p, carry):
            for par in range(2):
                j = g * 4 + 2 * p + par
                for i in range(4):
                    lhs = jnp.concatenate(
                        [lsrc[ch, :, i // 2, i % 2].reshape(NS * W, 128),
                         lsrc[ch, :, i // 2, 2].reshape(NS * W, 128)], axis=1)
                    img = jnp.dot(lhs, pp[j, pl.ds((h * 4 + i) * 256, 256), :],
                                  preferred_element_type=F32).astype(BF)
                    for s in range(NS):
                        li[pl.ds(i * W, W), pl.ds(s * 256, 256)] = img[s * W:(s + 1) * W]
                rows = pl.ds(64 - 64 * par, 256)
                rhs = jnp.concatenate(
                    [rsrc[ch, s, p, k, rows, :] for s in range(NS) for k in (par, 2)], axis=1)
                lanes = pl.ds(128 * par, 256)
                hr = pl.ds(h * 768, 768)
                acc[g, p, hr, lanes] += lax.dot_general(
                    li[...], rhs, (((1,), (1,)), ((), ())), preferred_element_type=F32)
            return carry

        lax.fori_loop(0, 2, pair, 0)

    def chunk(ch, carry):
        rectangle(ch, lown, rown, 0, 0)
        l_copy(ch).wait()
        r_copy(ch).wait()
        rectangle(ch, lfor, rown, 1, 0)
        rectangle(ch, lown, rfor, 0, 1)
        rectangle(ch, lfor, rfor, 1, 1)
        return carry

    lax.fori_loop(0, NC, chunk, 0)

    def d_copy(qi):
        l2, h = qi // 2, qi % 2
        rows = pl.ds(h * 768, 768)
        return pltpu.make_async_remote_copy(
            src_ref=acc.at[1 - c, l2, rows, :], dst_ref=drecv.at[l2, rows, :],
            send_sem=d_ss.at[qi], recv_sem=d_rs.at[qi], device_id=sib, device_id_type=MESH)

    rsb = (rs0, rs1, rs2, rs3)

    def rs_copy(qi, s):
        l2, h = qi // 2, qi % 2
        half = 384 >> s
        d = (qi + s) % 4
        send = offs[qi][s] + (1 - bits[d]) * half
        return pltpu.make_async_remote_copy(
            src_ref=acc.at[c, l2, pl.ds(pl.multiple_of(h * 768 + send, 16), half), :],
            dst_ref=rsb[s].at[qi], send_sem=rs_ss.at[qi, s], recv_sem=rs_rs.at[qi, s],
            device_id=dims[d], device_id_type=MESH)

    def add_rows(l2, first, src, src_first, rows):
        def step(k, carry):
            at = pl.ds(pl.multiple_of(first + k * 48, 16), 48)
            acc[c, l2, at, :] += src[pl.ds(pl.multiple_of(src_first + k * 48, 16), 48), :]
            return carry

        lax.fori_loop(0, rows // 48, step, 0)

    for qi in range(4):
        d_copy(qi).start()
    for qi in range(4):
        l2, h = qi // 2, qi % 2
        d_copy(qi).wait_recv()
        b = bits[qi]
        there = h * 768 + (1 - b) * 384
        here = h * 768 + b * 384
        add_rows(l2, there, drecv.at[l2], there, 384)
        rs_copy(qi, 0).start()
        add_rows(l2, here, drecv.at[l2], here, 384)

    def x_copy(l2):
        off = offs[l2 * 2 + 1][4]
        return pltpu.make_async_remote_copy(
            src_ref=acc.at[c, l2, pl.ds(pl.multiple_of(768 + off, 16), 48), :], dst_ref=xrecv.at[l2],
            send_sem=x_ss.at[l2], recv_sem=x_rs.at[l2], device_id=to_l, device_id_type=MESH)

    for s in range(4):
        for qi in range(4):
            l2, h = qi // 2, qi % 2
            rs_copy(qi, s).wait_recv()
            add_rows(l2, h * 768 + offs[qi][s + 1], rsb[s].at[qi], 0, 384 >> s)
            if s < 3:
                rs_copy(qi, s + 1).start()
            elif h == 1:
                x_copy(l2).start()

    def slab_rows(k, first, rows):
        return slabs_v.at[k, pl.ds(pl.multiple_of(first, 16), rows), :]

    def slab(qi):
        return (qi % 2) * 4 + c * 2 + qi // 2

    def ag_copy(qi, s):
        half = 384 >> s
        d = (qi + s) % 4
        ref = slab_rows(slab(qi), offs[qi][s + 1], half)
        return pltpu.make_async_remote_copy(
            src_ref=ref, dst_ref=ref, send_sem=ag_ss.at[qi, s], recv_sem=ag_rs.at[qi, s],
            device_id=dims[d], device_id_type=MESH)

    def fw_copy(qi, s):
        if s == 4:
            first, rows = offs[qi][4], 48
        else:
            rows = 384 >> s
            first = offs[qi][s] + (1 - bits[(qi + s) % 4]) * rows
        ref = slab_rows(slab(qi), first, rows)
        return pltpu.make_async_remote_copy(
            src_ref=ref, dst_ref=ref, send_sem=fw_ss.at[qi, s], recv_sem=fw_rs.at[qi, s],
            device_id=sib, device_id_type=MESH)

    sums = [jnp.zeros((1, 1), F32), jnp.zeros((1, 1), F32)]
    for qi in (0, 2, 1, 3):
        l2, t = qi // 2, qi % 2
        off = offs[qi][4]
        if t == 0:
            piece = acc[c, l2, pl.ds(pl.multiple_of(off, 16), 48), :]
        else:
            x_copy(l2).wait_recv()
            piece = xrecv[l2]
        full = piece + diag[qi]
        slabs_v[slab(qi), pl.ds(pl.multiple_of(off, 16), 48), :] = full.astype(BF)
        for m in range(2):
            sums[m] = sums[m] + jnp.sum(full * subp[qi, m], keepdims=True)
        ag_copy(qi, 3).start()
        fw_copy(qi, 4).start()

    lane = iota((8, 128), 1)
    pvs[0] = jnp.where(lane == 0, sums[0], jnp.where(lane == 1, sums[1], F32(0)))
    hops = (*dims, sib, to_l, to_r)

    def pv_copy(n):
        return pltpu.make_async_remote_copy(
            src_ref=pvs.at[n], dst_ref=pvr.at[n], send_sem=pv_ss.at[n], recv_sem=pv_rs.at[n],
            device_id=hops[n], device_id_type=MESH)

    def pv_step(n):
        pv_copy(n).wait_recv()
        pvs[n + 1] = pvs[n] + pvr[n]

    for s in (3, 2, 1, 0):
        n = 3 - s
        pv_copy(n).start()
        for qi in (0, 2, 1, 3):
            rows = 384 >> s
            first = offs[qi][s] + (1 - bits[(qi + s) % 4]) * rows
            ref = slab_rows(slab(qi), first, rows)
            pltpu.make_async_remote_copy(
                src_ref=ref, dst_ref=ref, send_sem=ag_ss.at[qi, s], recv_sem=ag_rs.at[qi, s],
                device_id=dims[(qi + s) % 4], device_id_type=MESH).wait_recv()
            if s > 0:
                ag_copy(qi, s - 1).start()
            fw_copy(qi, s).start()
        pv_step(n)

    def o_copy(k):
        return pltpu.make_async_copy(slab_rows(k, 0, 768), out_hbm.at[k], out_sem.at[k])

    for t in range(2):
        for l2 in range(2):
            o_copy(t * 4 + c * 2 + l2).start()
    for n in (4, 5, 6):
        pv_copy(n).start()
        pv_step(n)
    proj_out[...] = pvs[7]
    for qi in range(4):
        for s in range(5):
            if s == 4:
                first, rows = offs[qi][4], 48
            else:
                rows = 384 >> s
                first = offs[qi][s] + (1 - bits[(qi + s) % 4]) * rows
            ref = slab_rows((qi % 2) * 4 + (1 - c) * 2 + qi // 2, first, rows)
            pltpu.make_async_remote_copy(
                src_ref=ref, dst_ref=ref, send_sem=fw_ss.at[qi, s], recv_sem=fw_rs.at[qi, s],
                device_id=sib, device_id_type=MESH).wait_recv()
    for t in range(2):
        for l2 in range(2):
            o_copy(t * 4 + (1 - c) * 2 + l2).start()
    for qi in range(4):
        d_copy(qi).wait_send()
        for s in range(4):
            rs_copy(qi, s).wait_send()
            ag_copy(qi, s).wait_send()
        for s in range(5):
            fw_copy(qi, s).wait_send()
    for l2 in range(2):
        x_copy(l2).wait_send()
    for n in range(7):
        pv_copy(n).wait_send()
    for k in range(8):
        o_copy(k).wait()


def compact_body(rstart, rsize, src, out, total):
    x = lax.axis_index("site")
    x_l = x + 1 - 2 * (x % 2)
    rows = src.shape[1]
    total[...] = jnp.zeros_like(total)

    def one(k, carry):
        xt = jnp.where(k // 4 == 0, x, x_l)
        half = (k // 2) % 2
        site = xt + half * (3 - 2 * xt)
        q = site * 4 + 2 * (k % 2)
        start = rstart[q]
        base = pl.multiple_of(jnp.minimum((start // 128) * 128, BOND - 512), 128)
        j = iota((384, 512), 0)
        odd = j >= W
        idx = jnp.where(odd, j - W, j)
        size = jnp.where(odd, rsize[q + 1], rsize[q])
        first = jnp.where(odd, rstart[q + 1], start) - base
        hot = one_hot((idx < size) & (iota((384, 512), 1) == idx + first))
        total[:, pl.ds(base, 512)] += jnp.dot(src[k], hot, preferred_element_type=F32)
        return carry

    lax.fori_loop(0, 8, one, 0)
    out[...] = total[...].astype(BF)


def sector_tables(sector_ids, sectors):
    labels = jnp.arange(sectors, dtype=jnp.int32)
    starts = jnp.sum((sector_ids[None, :] < labels[:, None]).astype(jnp.int32), axis=1)
    sizes = jnp.sum((sector_ids[None, :] == labels[:, None]).astype(jnp.int32), axis=1)
    return starts, sizes


def local(wavefunction, left_blocks, right_blocks, left_sector, right_sector, term_count,
          left_energy, right_energy, subspace):
    lstart, lsize = sector_tables(left_sector, 16)
    rstart, rsize = sector_tables(right_sector, 16)
    smem = pl.BlockSpec(memory_space=pltpu.SMEM)
    vmem = pl.BlockSpec(memory_space=pltpu.VMEM)
    hbm = pl.BlockSpec(memory_space=pl.ANY)
    dma = pltpu.SemaphoreType.DMA
    big = pltpu.CompilerParams(vmem_limit_bytes=67043328)
    pp, diag, subp = pl.pallas_call(
        prep_body,
        out_shape=(jax.ShapeDtypeStruct((8, 2048, 256), BF), jax.ShapeDtypeStruct((4, 48, 384), F32),
                   jax.ShapeDtypeStruct((4, 2, 48, 384), F32)),
        in_specs=[smem] * 4 + [vmem] * 3 + [hbm],
        out_specs=(hbm, vmem, vmem),
        scratch_shapes=[
            pltpu.VMEM((2048, BOND), BF),
            pltpu.VMEM((8, 2048, 256), BF),
            pltpu.VMEM((4, 160, BOND), BF),
            dma((4, 2)), dma((8,)),
        ],
        compiler_params=big,
        name="prepare",
    )(lstart, lsize, rstart, rsize, wavefunction,
      left_energy.reshape(1, BOND), right_energy.reshape(1, BOND), subspace)
    slabs, proj = pl.pallas_call(
        body,
        out_shape=(jax.ShapeDtypeStruct((8, 768, 384), BF), jax.ShapeDtypeStruct((8, 128), F32)),
        in_specs=[smem] * 2 + [hbm] * 3 + [vmem] * 2,
        out_specs=(hbm, vmem),
        scratch_shapes=[
            pltpu.VMEM((8, 768, 384), BF),
            pltpu.VMEM((8, 2048, 256), BF),
            pltpu.VMEM((2, 2, NS, 4, W, W), BF),
            pltpu.VMEM((NC, NS, 2, 3, W, 128), BF),
            pltpu.VMEM((NC, NS, 2, 3, W, 128), BF),
            pltpu.VMEM((NC, NS, 2, 3, 320, 128), BF),
            pltpu.VMEM((NC, NS, 2, 3, 320, 128), BF),
            pltpu.VMEM((768, NS * 256), BF),
            pltpu.VMEM((2, 2, 1536, 384), F32),
            pltpu.VMEM((2, 1536, 384), F32),
            pltpu.VMEM((4, 384, 384), F32),
            pltpu.VMEM((4, 192, 384), F32),
            pltpu.VMEM((4, 96, 384), F32),
            pltpu.VMEM((4, 48, 384), F32),
            pltpu.VMEM((2, 48, 384), F32),
            pltpu.VMEM((8, 8, 128), F32),
            pltpu.VMEM((7, 8, 128), F32),
            dma((2, 2)), dma, dma((8,)),
            dma((NC,)), dma((NC,)), dma((NC,)), dma((NC,)),
            dma((4,)), dma((4,)), dma((4, 4)), dma((4, 4)), dma((2,)), dma((2,)),
            dma((4, 4)), dma((4, 4)), dma((4, 5)), dma((4, 5)), dma((7,)), dma((7,)),
        ],
        compiler_params=pltpu.CompilerParams(
            collective_id=0, has_side_effects=True, vmem_limit_bytes=67043328),
        name="exchange",
    )(lsize, term_count, pp, left_blocks, right_blocks, diag, subp)
    rows = 192
    sigma = pl.pallas_call(
        compact_body,
        grid=(768 // rows,),
        out_shape=jax.ShapeDtypeStruct((768, BOND), BF),
        in_specs=[smem, smem, pl.BlockSpec((8, rows, 384), lambda i: (0, i, 0))],
        out_specs=pl.BlockSpec((rows, BOND), lambda i: (i, 0)),
        scratch_shapes=[pltpu.VMEM((rows, BOND), F32)],
        name="compact",
    )(rstart, rsize, slabs)
    return sigma.reshape(4, W, BOND), proj[0, :2]


def solution(mesh):
    in_specs = (P(), P("ops", "site", None, None), P("ops", "site", None, None), P(), P(), P("ops"),
                P(), P(), P(None, "site", None, None))
    out_specs = (P("site", None, None), P())
    return jax.shard_map(local, mesh=mesh, in_specs=in_specs, out_specs=out_specs, check_vma=False)
```

```python
import jax
import jax.numpy as jnp
from jax import lax
from jax.experimental import pallas as pl
from jax.experimental.pallas import tpu as pltpu
from jax.sharding import PartitionSpec as P

W = 192
SLOTS = 8
NS = 2
NC = SLOTS // NS
BOND = 2048
BF = jnp.bfloat16
F32 = jnp.float32
MESH = pl.DeviceIdType.MESH


def iota(shape, dim):
    return lax.broadcasted_iota(jnp.int32, shape, dim)


def one_hot(mask):
    return jnp.where(mask, F32(1), F32(0)).astype(BF)


def packed_index(pos, parity):
    tail = pos - 64 * parity
    idx = jnp.where(pos < 128, pos, tail)
    ok = (pos < 128) | ((tail >= 128) & (tail < W))
    return idx, ok


CELLS = (
    ((0, ((0, 0), (0, 1))), (0, ((1, 0), (1, 1))), (0, ((0, 2), (1, 2))), (1, ((0, 0), (0, 1)))),
    ((0, ((0, 3), (1, 3))), (1, ((1, 0), (1, 1))), (1, ((0, 2), (1, 2))), (1, ((0, 3), (1, 3)))),
)
PLACE = {
    (h, l, r): (g, q, n)
    for g in range(2) for q, (h, pair) in enumerate(CELLS[g]) for n, (l, r) in enumerate(pair)
}
STEP = (192, 96, 48)


def piece_offsets(bits):
    offs = []
    for qi in range(4):
        off = [0]
        for s in range(3):
            off.append(off[-1] + bits[(qi + s) % 4] * STEP[s])
        offs.append(off)
    return offs


def cell_at(g, qi, n):
    (l0, r0), (l1, r1) = CELLS[g][qi][1]
    return l0 + n * (l1 - l0), r0 + n * (r1 - r0)


def label_bits(y, z):
    return (((y + 1) // 2) % 2, ((z + 1) // 2) % 2, y // 2, z // 2)


def prep_body(
    lstart, lsize, rstart, rsize, psi_v, lenergy, renergy, sub_hbm,
    pp_hbm, diag, subp, gath, pp, stack, sub_sem, pp_sem,
):
    x = lax.axis_index("site")
    o = lax.axis_index("ops")
    c = o % 2
    x_l = x + 1 - 2 * (x % 2)
    x_r = 3 - x
    offs = piece_offsets(label_bits((o // 2) % 4, o // 8))

    def piece(g, qi):
        off = offs[qi][3]
        n = off // W
        l, r = cell_at(g, qi, n)
        return 2 * l + c, off - n * W, r

    def sub_copy(g, qi, k):
        i, a0, r = piece(g, qi)
        return pltpu.make_async_copy(
            sub_hbm.at[k, i, pl.ds(pl.multiple_of(a0, 16), 48), :],
            stack.at[g * 4 + qi, pl.ds(48 + 48 * k, 48), :], sub_sem.at[g * 4 + qi, k])

    for g in range(2):
        for qi in range(4):
            for k in range(2):
                sub_copy(g, qi, k).start()

    def row_hot(q, first, rows, packed):
        rs = lstart[q]
        base = pl.multiple_of(jnp.minimum((rs // 16) * 16, BOND - 256), 16)
        pos = iota((rows, 256), 0) + first
        if packed:
            idx, ok = packed_index(pos, q % 2)
        else:
            idx, ok = pos, pos < W
        ok = ok & (idx < lsize[q])
        return base, one_hot(ok & (iota((rows, 256), 1) == idx + (rs - base)))

    def rows_of(i, carry):
        q = jnp.where(i < 4, x * 4 + i, x_l * 4 + i - 4)
        base, hot = row_hot(q, 0, 256, True)
        for n in range(4):
            win = psi_v[pl.ds(base, 256), pl.ds(n * 512, 512)]
            gath[pl.ds(pl.multiple_of(i * 256, 256), 256), pl.ds(n * 512, 512)] = jnp.dot(
                hot, win, preferred_element_type=F32).astype(BF)
        return carry

    lax.fori_loop(0, 8, rows_of, 0)

    def pp_copy(j):
        return pltpu.make_async_copy(pp.at[j], pp_hbm.at[j], pp_sem.at[j])

    def cols_of(j, carry):
        q = jnp.where(j < 4, x * 4 + j, x_r * 4 + j - 4)
        cs = rstart[q]
        cb = pl.multiple_of(jnp.minimum((cs // 128) * 128, BOND - 384), 128)
        idx, ok = packed_index(iota((384, 256), 1), q % 2)
        ok = ok & (idx < rsize[q])
        hot = one_hot(ok & (iota((384, 256), 0) == idx + (cs - cb)))
        for m in range(4):
            win = gath[pl.ds(m * 512, 512), pl.ds(cb, 384)]
            pp[j, pl.ds(m * 512, 512), :] = jnp.dot(win, hot, preferred_element_type=F32).astype(BF)
        pp_copy(j).start()
        return carry

    lax.fori_loop(0, 8, cols_of, 0)

    re = renergy[...]
    hi = re.astype(BF)
    rem = re - hi.astype(F32)
    mid = rem.astype(BF)
    low = (rem - mid.astype(F32)).astype(BF)
    rows16 = iota((16, BOND), 0)
    er3 = jnp.where(rows16 == 0, hi.astype(F32),
                    jnp.where(rows16 == 1, mid.astype(F32),
                              jnp.where(rows16 == 2, low.astype(F32), F32(0)))).astype(BF)
    for g in range(2):
        for qi in range(4):
            at = g * 4 + qi
            i, a0, r = piece(g, qi)
            q = x * 4 + i
            base, hot = row_hot(q, a0, 48, False)
            for n in range(4):
                win = psi_v[pl.ds(base, 256), pl.ds(n * 512, 512)]
                stack[at, pl.ds(0, 48), pl.ds(n * 512, 512)] = jnp.dot(
                    hot, win, preferred_element_type=F32).astype(BF)
            stack[at, pl.ds(144, 16), :] = er3
            for k in range(2):
                sub_copy(g, qi, k).wait()
            xt = x if CELLS[g][qi][0] == 0 else x_l
            site = xt + (r // 2) * (3 - 2 * xt)
            total = None
            for par in range(2):
                qr = site * 4 + 2 * (r % 2) + par
                cs = rstart[qr]
                cb = pl.multiple_of(jnp.minimum((cs // 128) * 128, BOND - 384), 128)
                j = iota((384, 384), 1) - W * par
                hot2 = one_hot((j >= 0) & (j < W) & (j < rsize[qr]) & (iota((384, 384), 0) == j + (cs - cb)))
                part = jnp.dot(stack[at, :, pl.ds(cb, 384)], hot2, preferred_element_type=F32)
                total = part if total is None else total + part
            lb = pl.multiple_of(jnp.minimum((lstart[q] // 128) * 128, BOND - 384), 128)
            shift = lstart[q] - lb + a0
            pick = iota((48, 384), 1) == iota((48, 384), 0) + shift
            el = jnp.sum(jnp.where(pick, lenergy[:, pl.ds(lb, 384)], F32(0)), axis=1, keepdims=True)
            er = total[144:145] + total[145:146] + total[146:147]
            diag[at] = (el + er) * total[:48]
            subp[at, 0] = total[48:96]
            subp[at, 1] = total[96:144]

    for j in range(8):
        pp_copy(j).wait()


def body(
    lsize, count, pp_hbm, left_hbm, right_hbm, diag, subp,
    out_hbm, proj_out,
    slabs, pp, raw, lown, lfor, rown, rfor, li, acc,
    drecv, rs0, rs1, rs2, rs3, xrecv, pvs, pvr,
    raw_sem, pp_sem, out_sem,
    l_ss, l_rs, r_ss, r_rs, d_ss, d_rs, rs_ss, rs_rs, x_ss, x_rs,
    ag_ss, ag_rs, fw_ss, fw_rs, pv_ss, pv_rs,
):
    x = lax.axis_index("site")
    o = lax.axis_index("ops")
    c = o % 2
    y = (o // 2) % 4
    z = o // 8
    x_l = x + 1 - 2 * (x % 2)
    x_r = 3 - x
    to_l = {"site": x_l}
    to_r = {"site": x_r}
    sib = {"ops": o + 1 - 2 * c}
    y_a = y + 1 - 2 * (y % 2)
    z_a = z + 1 - 2 * (z % 2)
    y_c = 3 - y_a
    z_c = 3 - z_a
    x_c = 3 - x_l
    dims = (
        {"ops": o + 2 * (y_a - y)},
        {"ops": o + 8 * (z_a - z)},
        {"ops": o + 2 * (3 - 2 * y)},
        {"ops": o + 8 * (3 - 2 * z)},
    )
    far = ({"ops": o + 2 * (y_c - y)}, {"ops": o + 8 * (z_c - z)}, {"site": x_c})
    bits = label_bits(y, z)
    offs = piece_offsets(bits)

    def raw_copies(m):
        buf = m % 2
        return (
            pltpu.make_async_copy(left_hbm.at[pl.ds(NS * m, NS)], raw.at[buf, 0], raw_sem.at[buf, 0]),
            pltpu.make_async_copy(right_hbm.at[pl.ds(NS * m, NS)], raw.at[buf, 1], raw_sem.at[buf, 1]),
        )

    for m in range(2):
        for cp in raw_copies(m):
            cp.start()
    pp_copy = pltpu.make_async_copy(pp_hbm, pp, pp_sem)
    pp_copy.start()

    pvr[...] = jnp.zeros_like(pvr)
    barrier = pltpu.get_barrier_semaphore()
    for who in (to_l, to_r, sib, *dims, *far):
        pl.semaphore_signal(barrier, inc=1, device_id=who, device_id_type=MESH)

    zrow = jnp.zeros((2, SLOTS, 3, 64, 128), BF)
    for buf in (rown, rfor):
        for start in (0, 256):
            buf[:, :, :, pl.ds(start, 64), :] = zrow

    def l_copy(p, m):
        at = pl.ds(NS * m, NS)
        return pltpu.make_async_remote_copy(
            src_ref=lown.at[p, at], dst_ref=lfor.at[p, at], send_sem=l_ss.at[p, m], recv_sem=l_rs.at[p, m],
            device_id=to_l, device_id_type=MESH)

    def r_copy(p, m):
        at = pl.ds(NS * m, NS)
        rows = pl.ds(64, W)
        return pltpu.make_async_remote_copy(
            src_ref=rown.at[p, at, :, rows, :], dst_ref=rfor.at[p, at, :, rows, :],
            send_sem=r_ss.at[p, m], recv_sem=r_rs.at[p, m], device_id=to_r, device_id_type=MESH)

    def pack(m):
        buf = m % 2

        def one(k, carry):
            s = k // 2
            p = k % 2
            slot = NS * m + s
            row = iota((W, 128), 0)
            live = slot < count[0]
            keep = []
            for par in range(2):
                size = jnp.where(live, lsize[x * 4 + 2 * p + par], 0)
                keep.append(one_hot(row < size))
            ev = raw[buf, 0, s, 2 * p]
            od = raw[buf, 0, s, 2 * p + 1]
            lown[p, slot, 0] = ev[:, :128] * keep[0]
            lown[p, slot, 1] = od[:, :128] * keep[1]
            lown[p, slot, 2] = jnp.concatenate(
                [ev[:, 128:] * keep[0][:, :64], od[:, 128:] * keep[1][:, :64]], axis=1)
            ev = raw[buf, 1, s, 2 * p]
            od = raw[buf, 1, s, 2 * p + 1]
            rows = pl.ds(64, W)
            rown[p, slot, 0, rows, :] = ev[:, :128]
            rown[p, slot, 1, rows, :] = od[:, :128]
            rown[p, slot, 2, rows, :] = jnp.concatenate([ev[:, 128:], od[:, 128:]], axis=1)
            return carry

        lax.fori_loop(0, 2 * NS, one, 0)

    for m in range(NC):
        for cp in raw_copies(m):
            cp.wait()
        pack(m)
        if m == 0:
            pl.semaphore_wait(barrier, 10)
        if m + 2 < NC:
            for cp in raw_copies(m + 2):
                cp.start()
        l_copy(0, m).start()
        r_copy(0, m).start()
    for m in range(NC):
        l_copy(1, m).start()
        r_copy(1, m).start()

    def clear(k, carry):
        for g in range(2):
            for q in range(4):
                acc[g, q, k // 2, pl.ds(pl.multiple_of((k % 2) * W, W), W), :] = jnp.zeros((W, 384), F32)
        return carry

    lax.fori_loop(0, 4, clear, 0)
    pp_copy.wait()

    def product(m, r, lefts):
        rsrc = rown if r < 2 else rfor
        slots = pl.ds(NS * m, NS)
        for par in range(2):
            j = 2 * r + par
            for n, (h, l) in enumerate(lefts):
                lsrc = lown if h == 0 else lfor
                tail = lsrc[l, slots, 2].reshape(NS * W, 128)
                for pa in range(2):
                    lhs = jnp.concatenate([lsrc[l, slots, pa].reshape(NS * W, 128), tail], axis=1)
                    img = jnp.dot(lhs, pp[j, pl.ds((h * 4 + 2 * l + pa) * 256, 256), :],
                                  preferred_element_type=F32).astype(BF)
                    for s in range(NS):
                        li[pl.ds((2 * n + pa) * W, W), pl.ds(s * 256, 256)] = img[s * W:(s + 1) * W]
            rows = pl.ds(64 - 64 * par, 256)
            rhs = jnp.concatenate(
                [rsrc[r % 2, NS * m + s, k, rows, :] for s in range(NS) for k in (par, 2)], axis=1)
            lanes = pl.ds(128 * par, 256)
            for n, (h, l) in enumerate(lefts):
                g, q, cell = PLACE[(h, l, r)]
                res = lax.dot_general(li[pl.ds(2 * n * W, 2 * W), :], rhs, (((1,), (1,)), ((), ())),
                                      preferred_element_type=F32)
                for pa in range(2):
                    acc[g, q, pa, pl.ds(cell * W, W), lanes] += res[pa * W:(pa + 1) * W]

    def arrive(p, m):
        l_copy(p, m).wait()
        r_copy(p, m).wait()

    def d_copy(g, qi):
        return pltpu.make_async_remote_copy(
            src_ref=acc.at[g, qi, 1 - c], dst_ref=drecv.at[g, qi],
            send_sem=d_ss.at[g, qi], recv_sem=d_rs.at[g, qi], device_id=sib, device_id_type=MESH)

    rsb = (rs0, rs1, rs2, rs3)

    def rs_copy(g, qi, s):
        d = (qi + s) % 4
        if s < 3:
            rows = STEP[s]
            first = offs[qi][s] + (1 - bits[d]) * rows
        else:
            rows, first = 48, offs[qi][3]
        return pltpu.make_async_remote_copy(
            src_ref=acc.at[g, qi, c, pl.ds(pl.multiple_of(first, 16), rows), :],
            dst_ref=rsb[s].at[g, qi], send_sem=rs_ss.at[g, qi, s], recv_sem=rs_rs.at[g, qi, s],
            device_id=dims[d], device_id_type=MESH)

    def add_rows(g, qi, first, src, src_first, rows):
        def step(k, carry):
            at = pl.ds(pl.multiple_of(first + k * 48, 16), 48)
            acc[g, qi, c, at, :] += src[pl.ds(pl.multiple_of(src_first + k * 48, 16), 48), :]
            return carry

        lax.fori_loop(0, rows // 48, step, 0)

    def core_sum(g):
        for qi in range(4):
            d_copy(g, qi).wait_recv()
            there = (1 - bits[qi]) * 192
            here = bits[qi] * 192
            add_rows(g, qi, there, drecv.at[g, qi], there, 192)
            rs_copy(g, qi, 0).start()
            add_rows(g, qi, here, drecv.at[g, qi], here, 192)

    def x_copy(g, qi):
        return pltpu.make_async_remote_copy(
            src_ref=acc.at[g, qi, c, pl.ds(pl.multiple_of(offs[qi][3], 16), 48), :], dst_ref=xrecv.at[g, qi],
            send_sem=x_ss.at[g, qi], recv_sem=x_rs.at[g, qi], device_id=to_l, device_id_type=MESH)

    def reduce_step(g, s):
        for qi in range(4):
            rs_copy(g, qi, s).wait_recv()
            if s == 3:
                rs_copy(g, qi, 3).wait_send()
                add_rows(g, qi, offs[qi][3], rs3.at[g, qi], 0, 48)
                if CELLS[g][qi][0] == 1:
                    x_copy(g, qi).start()
            else:
                add_rows(g, qi, offs[qi][s + 1], rsb[s].at[g, qi], 0, STEP[s])
                rs_copy(g, qi, s + 1).start()

    def rows_at(g, qi, first, rows, core):
        n = first // W
        l, r = cell_at(g, qi, n)
        at = (2 * l + core) * W + first - n * W
        return CELLS[g][qi][0] * 4 + r, pl.ds(pl.multiple_of(at, 16), rows)

    def ag_copy(g, qi, s, mine):
        d = (qi + s) % 4
        first = offs[qi][s + 1] if mine else offs[qi][s] + (1 - bits[d]) * STEP[s]
        k, at = rows_at(g, qi, first, STEP[s], c)
        return pltpu.make_async_remote_copy(
            src_ref=slabs.at[k, at, :], dst_ref=slabs.at[k, at, :],
            send_sem=ag_ss.at[g, qi, s], recv_sem=ag_rs.at[g, qi, s],
            device_id=dims[d], device_id_type=MESH)

    def fw_copy(g, qi, s, core):
        if s == 3:
            first, rows = offs[qi][3], 48
        else:
            first, rows = offs[qi][s] + (1 - bits[(qi + s) % 4]) * STEP[s], STEP[s]
        k, at = rows_at(g, qi, first, rows, core)
        return pltpu.make_async_remote_copy(
            src_ref=slabs.at[k, at, :], dst_ref=slabs.at[k, at, :],
            send_sem=fw_ss.at[g, qi, s], recv_sem=fw_rs.at[g, qi, s],
            device_id=sib, device_id_type=MESH)

    sums = [jnp.zeros((1, 1), F32), jnp.zeros((1, 1), F32)]

    def finish(g, h):
        for qi in range(4):
            if CELLS[g][qi][0] != h:
                continue
            off = offs[qi][3]
            if h == 0:
                part = acc[g, qi, c, pl.ds(pl.multiple_of(off, 16), 48), :]
            else:
                x_copy(g, qi).wait_recv()
                part = xrecv[g, qi]
            full = part + diag[g * 4 + qi]
            k, at = rows_at(g, qi, off, 48, c)
            slabs[k, at, :] = full.astype(BF)
            ag_copy(g, qi, 2, True).start()
            fw_copy(g, qi, 3, c).start()
            weight = (1 - bits[(qi + 3) % 4]).astype(F32)
            for k in range(2):
                sums[k] = sums[k] + weight * jnp.sum(full * subp[g * 4 + qi, k], keepdims=True)

    def gather_step(g, s, h=None):
        for qi in range(4):
            if h is not None and CELLS[g][qi][0] != h:
                continue
            ag_copy(g, qi, s, False).wait_recv()
            if s > 0:
                ag_copy(g, qi, s - 1, True).start()
            fw_copy(g, qi, s, c).start()

    def step0(m, carry):
        for r in range(2):
            product(m, r, ((0, 0), (0, 1)))
        return carry

    lax.fori_loop(0, NC, step0, 0)

    def step1(m, carry):
        arrive(0, m)
        for r in range(2):
            product(m, r, ((1, 0),))
        product(m, 2, ((0, 0), (0, 1), (1, 0)))
        return carry

    lax.fori_loop(0, NC, step1, 0)
    for qi in range(4):
        d_copy(0, qi).start()

    def first_half(m):
        arrive(1, m)
        for r in range(3):
            product(m, r, ((1, 1),))

    def second_half(m):
        product(m, 3, ((0, 0), (0, 1), (1, 0), (1, 1)))

    first_half(0)
    core_sum(0)
    second_half(0)
    first_half(1)
    reduce_step(0, 0)
    second_half(1)
    reduce_step(0, 1)
    first_half(2)
    reduce_step(0, 2)
    second_half(2)
    reduce_step(0, 3)
    finish(0, 0)
    first_half(3)
    for qi in (1, 2):
        d_copy(1, qi).start()
    second_half(3)
    for qi in (0, 3):
        d_copy(1, qi).start()
    finish(0, 1)
    gather_step(0, 2)
    core_sum(1)
    gather_step(0, 1)
    reduce_step(1, 0)
    gather_step(0, 0)
    reduce_step(1, 1)
    reduce_step(1, 2)
    reduce_step(1, 3)
    finish(1, 0)
    finish(1, 1)

    lane = iota((8, 128), 1)
    pvs[0] = jnp.where(lane == 0, sums[0], jnp.where(lane == 1, sums[1], F32(0)))
    rounds = (
        (c, ((sib, 1 - c),)),
        (y, ((dims[0], y_a), (dims[2], 3 - y), (far[0], y_c))),
        (z, ((dims[1], z_a), (dims[3], 3 - z), (far[1], z_c))),
        (x, ((to_l, x_l), (to_r, x_r), (far[2], x_c))),
    )

    def pv_copy(n, i, slot):
        return pltpu.make_async_remote_copy(
            src_ref=pvs.at[n], dst_ref=pvr.at[n, slot], send_sem=pv_ss.at[n, i], recv_sem=pv_rs.at[n, slot],
            device_id=rounds[n][1][i][0], device_id_type=MESH)

    def pv_send(n):
        me, others = rounds[n]
        for i in range(len(others)):
            pv_copy(n, i, me).start()
        pvr[n, me] = pvs[n]

    def pv_sum(n):
        me, others = rounds[n]
        for i, (who, slot) in enumerate(others):
            pv_copy(n, i, slot).wait_recv()
        pvs[n + 1] = (pvr[n, 0] + pvr[n, 1]) + (pvr[n, 2] + pvr[n, 3])

    def o_copy(k, core):
        rows = tuple(pl.ds((2 * l + core) * W, W) for l in range(2))
        return [pltpu.make_async_copy(slabs.at[k, at, :], out_hbm.at[k, at, :], out_sem.at[k, core, l])
                for l, at in enumerate(rows)]

    pv_send(0)
    for n, s in enumerate((2, 1, 0)):
        gather_step(1, s)
        pv_sum(n)
        pv_send(n + 1)
    for k in range(8):
        for cp in o_copy(k, c):
            cp.start()
    for g in range(2):
        for s in (3, 2, 1, 0):
            for qi in range(4):
                fw_copy(g, qi, s, 1 - c).wait_recv()
    for k in range(8):
        for cp in o_copy(k, 1 - c):
            cp.start()
    pv_sum(3)
    proj_out[...] = pvs[4]
    for g in range(2):
        for qi in range(4):
            d_copy(g, qi).wait_send()
            for s in range(3):
                rs_copy(g, qi, s).wait_send()
                ag_copy(g, qi, s, True).wait_send()
            for s in range(4):
                fw_copy(g, qi, s, c).wait_send()
            if CELLS[g][qi][0] == 1:
                x_copy(g, qi).wait_send()
    for n in range(4):
        for i in range(len(rounds[n][1])):
            pv_copy(n, i, rounds[n][0]).wait_send()
    for k in range(8):
        for core in (c, 1 - c):
            for cp in o_copy(k, core):
                cp.wait()


def compact_body(rstart, rsize, src, out):
    x = lax.axis_index("site")
    k = pl.program_id(0)
    x_l = x + 1 - 2 * (x % 2)

    @pl.when(k == 0)
    def _():
        out[...] = jnp.zeros_like(out)

    xt = jnp.where(k // 4 == 0, x, x_l)
    site = xt + ((k // 2) % 2) * (3 - 2 * xt)
    q = site * 4 + 2 * (k % 2)
    start = rstart[q]
    base = pl.multiple_of(jnp.minimum((start // 128) * 128, BOND - 512), 128)
    j = iota((384, 512), 0)
    odd = j >= W
    idx = jnp.where(odd, j - W, j)
    size = jnp.where(odd, rsize[q + 1], rsize[q])
    first = jnp.where(odd, rstart[q + 1], start) - base
    hot = one_hot((idx < size) & (iota((384, 512), 1) == idx + first))
    out[:, pl.ds(base, 512)] += jnp.dot(src[0], hot, preferred_element_type=F32).astype(BF)


def sector_tables(sector_ids, sectors):
    labels = jnp.arange(sectors, dtype=jnp.int32)
    starts = jnp.sum((sector_ids[None, :] < labels[:, None]).astype(jnp.int32), axis=1)
    sizes = jnp.sum((sector_ids[None, :] == labels[:, None]).astype(jnp.int32), axis=1)
    return starts, sizes


def local(wavefunction, left_blocks, right_blocks, left_sector, right_sector, term_count,
          left_energy, right_energy, subspace):
    lstart, lsize = sector_tables(left_sector, 16)
    rstart, rsize = sector_tables(right_sector, 16)
    smem = pl.BlockSpec(memory_space=pltpu.SMEM)
    vmem = pl.BlockSpec(memory_space=pltpu.VMEM)
    hbm = pl.BlockSpec(memory_space=pl.ANY)
    dma = pltpu.SemaphoreType.DMA
    big = pltpu.CompilerParams(vmem_limit_bytes=67043328)
    pp, diag, subp = pl.pallas_call(
        prep_body,
        out_shape=(jax.ShapeDtypeStruct((8, 2048, 256), BF), jax.ShapeDtypeStruct((8, 48, 384), F32),
                   jax.ShapeDtypeStruct((8, 2, 48, 384), F32)),
        in_specs=[smem] * 4 + [vmem] * 3 + [hbm],
        out_specs=(hbm, vmem, vmem),
        scratch_shapes=[
            pltpu.VMEM((2048, BOND), BF),
            pltpu.VMEM((8, 2048, 256), BF),
            pltpu.VMEM((8, 160, BOND), BF),
            dma((8, 2)), dma((8,)),
        ],
        compiler_params=big,
        name="prepare",
    )(lstart, lsize, rstart, rsize, wavefunction,
      left_energy.reshape(1, BOND), right_energy.reshape(1, BOND), subspace)
    slabs, proj = pl.pallas_call(
        body,
        out_shape=(jax.ShapeDtypeStruct((8, 768, 384), BF), jax.ShapeDtypeStruct((8, 128), F32)),
        in_specs=[smem] * 2 + [hbm] * 3 + [vmem] * 2,
        out_specs=(hbm, vmem),
        scratch_shapes=[
            pltpu.VMEM((8, 768, 384), BF),
            pltpu.VMEM((8, 2048, 256), BF),
            pltpu.VMEM((2, 2, NS, 4, W, W), BF),
            pltpu.VMEM((2, SLOTS, 3, W, 128), BF),
            pltpu.VMEM((2, SLOTS, 3, W, 128), BF),
            pltpu.VMEM((2, SLOTS, 3, 320, 128), BF),
            pltpu.VMEM((2, SLOTS, 3, 320, 128), BF),
            pltpu.VMEM((1536, NS * 256), BF),
            pltpu.VMEM((2, 4, 2, 384, 384), F32),
            pltpu.VMEM((2, 4, 384, 384), F32),
            pltpu.VMEM((2, 4, 192, 384), F32),
            pltpu.VMEM((2, 4, 96, 384), F32),
            pltpu.VMEM((2, 4, 48, 384), F32),
            pltpu.VMEM((2, 4, 48, 384), F32),
            pltpu.VMEM((2, 4, 48, 384), F32),
            pltpu.VMEM((5, 8, 128), F32),
            pltpu.VMEM((4, 4, 8, 128), F32),
            dma((2, 2)), dma, dma((8, 2, 2)),
            dma((2, NC)), dma((2, NC)), dma((2, NC)), dma((2, NC)),
            dma((2, 4)), dma((2, 4)), dma((2, 4, 4)), dma((2, 4, 4)), dma((2, 4)), dma((2, 4)),
            dma((2, 4, 3)), dma((2, 4, 3)), dma((2, 4, 4)), dma((2, 4, 4)), dma((4, 3)), dma((4, 4)),
        ],
        compiler_params=pltpu.CompilerParams(
            collective_id=0, has_side_effects=True, vmem_limit_bytes=67043328),
        name="exchange",
    )(lsize, term_count, pp, left_blocks, right_blocks, diag, subp)
    sigma = pl.pallas_call(
        compact_body,
        grid=(8,),
        out_shape=jax.ShapeDtypeStruct((768, BOND), BF),
        in_specs=[smem, smem, pl.BlockSpec((1, 768, 384), lambda k: (k, 0, 0))],
        out_specs=pl.BlockSpec((768, BOND), lambda k: (0, 0)),
        name="compact",
    )(rstart, rsize, slabs)
    return sigma.reshape(4, W, BOND), proj[0, :2]


def solution(mesh):
    in_specs = (P(), P("ops", "site", None, None), P("ops", "site", None, None), P(), P(), P("ops"),
                P(), P(), P(None, "site", None, None))
    out_specs = (P("site", None, None), P())
    return jax.shard_map(local, mesh=mesh, in_specs=in_specs, out_specs=out_specs, check_vma=False)
```

```python
import jax
import jax.numpy as jnp
from jax import lax
from jax.experimental import pallas as pl
from jax.experimental.pallas import tpu as pltpu
from jax.sharding import PartitionSpec as P

W = 192
SLOTS = 8
NS = 2
NC = SLOTS // NS
BOND = 2048
BF = jnp.bfloat16
F32 = jnp.float32
MESH = pl.DeviceIdType.MESH


def iota(shape, dim):
    return lax.broadcasted_iota(jnp.int32, shape, dim)


def one_hot(mask):
    return jnp.where(mask, F32(1), F32(0)).astype(BF)


def packed_index(pos, parity):
    tail = pos - 64 * parity
    idx = jnp.where(pos < 128, pos, tail)
    ok = (pos < 128) | ((tail >= 128) & (tail < W))
    return idx, ok


CELLS = (
    ((0, ((0, 0), (0, 1))), (0, ((1, 0), (1, 1))), (0, ((0, 2), (1, 2))), (1, ((0, 0), (0, 1)))),
    ((0, ((0, 3), (1, 3))), (1, ((1, 0), (1, 1))), (1, ((0, 2), (1, 2))), (1, ((0, 3), (1, 3)))),
)
PLACE = {
    (h, l, r): (g, q, n)
    for g in range(2) for q, (h, pair) in enumerate(CELLS[g]) for n, (l, r) in enumerate(pair)
}
STEP = (192, 96, 48)


def piece_offsets(bits):
    offs = []
    for qi in range(4):
        off = [0]
        for s in range(3):
            off.append(off[-1] + bits[(qi + s) % 4] * STEP[s])
        offs.append(off)
    return offs


def cell_at(g, qi, n):
    (l0, r0), (l1, r1) = CELLS[g][qi][1]
    return l0 + n * (l1 - l0), r0 + n * (r1 - r0)


def label_bits(y, z):
    return (((y + 1) // 2) % 2, ((z + 1) // 2) % 2, y // 2, z // 2)


def prep_body(
    lstart, lsize, rstart, rsize, psi_v, lenergy, renergy, sub_hbm,
    pp_hbm, diag, subp, gath, pp, stack, sub_sem, pp_sem,
):
    x = lax.axis_index("site")
    o = lax.axis_index("ops")
    c = o % 2
    x_l = x + 1 - 2 * (x % 2)
    x_r = 3 - x
    offs = piece_offsets(label_bits((o // 2) % 4, o // 8))

    def piece(g, qi):
        off = offs[qi][3]
        n = off // W
        l, r = cell_at(g, qi, n)
        return 2 * l + c, off - n * W, r

    def sub_copy(g, qi, k):
        i, a0, r = piece(g, qi)
        return pltpu.make_async_copy(
            sub_hbm.at[k, i, pl.ds(pl.multiple_of(a0, 16), 48), :],
            stack.at[g * 4 + qi, pl.ds(48 + 48 * k, 48), :], sub_sem.at[g * 4 + qi, k])

    for g in range(2):
        for qi in range(4):
            for k in range(2):
                sub_copy(g, qi, k).start()

    def row_hot(q, first, rows, packed):
        rs = lstart[q]
        base = pl.multiple_of(jnp.minimum((rs // 16) * 16, BOND - 256), 16)
        pos = iota((rows, 256), 0) + first
        if packed:
            idx, ok = packed_index(pos, q % 2)
        else:
            idx, ok = pos, pos < W
        ok = ok & (idx < lsize[q])
        return base, one_hot(ok & (iota((rows, 256), 1) == idx + (rs - base)))

    def rows_of(i, carry):
        q = jnp.where(i < 4, x * 4 + i, x_l * 4 + i - 4)
        base, hot = row_hot(q, 0, 256, True)
        for n in range(4):
            win = psi_v[pl.ds(base, 256), pl.ds(n * 512, 512)]
            gath[pl.ds(pl.multiple_of(i * 256, 256), 256), pl.ds(n * 512, 512)] = jnp.dot(
                hot, win, preferred_element_type=F32).astype(BF)
        return carry

    lax.fori_loop(0, 8, rows_of, 0)

    def pp_copy(j):
        return pltpu.make_async_copy(pp.at[j], pp_hbm.at[j], pp_sem.at[j])

    def cols_of(j, carry):
        q = jnp.where(j < 4, x * 4 + j, x_r * 4 + j - 4)
        cs = rstart[q]
        cb = pl.multiple_of(jnp.minimum((cs // 128) * 128, BOND - 384), 128)
        idx, ok = packed_index(iota((384, 256), 1), q % 2)
        ok = ok & (idx < rsize[q])
        hot = one_hot(ok & (iota((384, 256), 0) == idx + (cs - cb)))
        for m in range(4):
            win = gath[pl.ds(m * 512, 512), pl.ds(cb, 384)]
            pp[j, pl.ds(m * 512, 512), :] = jnp.dot(win, hot, preferred_element_type=F32).astype(BF)
        pp_copy(j).start()
        return carry

    lax.fori_loop(0, 8, cols_of, 0)

    re = renergy[...]
    hi = re.astype(BF)
    rem = re - hi.astype(F32)
    mid = rem.astype(BF)
    low = (rem - mid.astype(F32)).astype(BF)
    rows16 = iota((16, BOND), 0)
    er3 = jnp.where(rows16 == 0, hi.astype(F32),
                    jnp.where(rows16 == 1, mid.astype(F32),
                              jnp.where(rows16 == 2, low.astype(F32), F32(0)))).astype(BF)
    for g in range(2):
        for qi in range(4):
            at = g * 4 + qi
            i, a0, r = piece(g, qi)
            q = x * 4 + i
            base, hot = row_hot(q, a0, 48, False)
            for n in range(4):
                win = psi_v[pl.ds(base, 256), pl.ds(n * 512, 512)]
                stack[at, pl.ds(0, 48), pl.ds(n * 512, 512)] = jnp.dot(
                    hot, win, preferred_element_type=F32).astype(BF)
            stack[at, pl.ds(144, 16), :] = er3
            for k in range(2):
                sub_copy(g, qi, k).wait()
            xt = x if CELLS[g][qi][0] == 0 else x_l
            site = xt + (r // 2) * (3 - 2 * xt)
            total = None
            for par in range(2):
                qr = site * 4 + 2 * (r % 2) + par
                cs = rstart[qr]
                cb = pl.multiple_of(jnp.minimum((cs // 128) * 128, BOND - 384), 128)
                j = iota((384, 384), 1) - W * par
                hot2 = one_hot((j >= 0) & (j < W) & (j < rsize[qr]) & (iota((384, 384), 0) == j + (cs - cb)))
                part = jnp.dot(stack[at, :, pl.ds(cb, 384)], hot2, preferred_element_type=F32)
                total = part if total is None else total + part
            lb = pl.multiple_of(jnp.minimum((lstart[q] // 128) * 128, BOND - 384), 128)
            shift = lstart[q] - lb + a0
            pick = iota((48, 384), 1) == iota((48, 384), 0) + shift
            el = jnp.sum(jnp.where(pick, lenergy[:, pl.ds(lb, 384)], F32(0)), axis=1, keepdims=True)
            er = total[144:145] + total[145:146] + total[146:147]
            diag[at] = (el + er) * total[:48]
            subp[at, 0] = total[48:96]
            subp[at, 1] = total[96:144]

    for j in range(8):
        pp_copy(j).wait()


def body(
    lsize, count, pp_hbm, left_hbm, right_hbm, diag, subp,
    out_hbm, proj_out,
    slabs, pp, raw, lown, lfor, rown, rfor, li, acc,
    drecv, rs0, rs1, rs2, rs3, xrecv, pvs, pvr,
    raw_sem, pp_sem, out_sem,
    l_ss, l_rs, r_ss, r_rs, d_ss, d_rs, rs_ss, rs_rs, x_ss, x_rs,
    ag_ss, ag_rs, fw_ss, fw_rs, pv_ss, pv_rs,
):
    x = lax.axis_index("site")
    o = lax.axis_index("ops")
    c = o % 2
    y = (o // 2) % 4
    z = o // 8
    x_l = x + 1 - 2 * (x % 2)
    x_r = 3 - x
    to_l = {"site": x_l}
    to_r = {"site": x_r}
    sib = {"ops": o + 1 - 2 * c}
    y_a = y + 1 - 2 * (y % 2)
    z_a = z + 1 - 2 * (z % 2)
    y_c = 3 - y_a
    z_c = 3 - z_a
    x_c = 3 - x_l
    dims = (
        {"ops": o + 2 * (y_a - y)},
        {"ops": o + 8 * (z_a - z)},
        {"ops": o + 2 * (3 - 2 * y)},
        {"ops": o + 8 * (3 - 2 * z)},
    )
    far = ({"ops": o + 2 * (y_c - y)}, {"ops": o + 8 * (z_c - z)}, {"site": x_c})
    bits = label_bits(y, z)
    offs = piece_offsets(bits)

    def raw_copies(m):
        buf = m % 2
        return (
            pltpu.make_async_copy(left_hbm.at[pl.ds(NS * m, NS)], raw.at[buf, 0], raw_sem.at[buf, 0]),
            pltpu.make_async_copy(right_hbm.at[pl.ds(NS * m, NS)], raw.at[buf, 1], raw_sem.at[buf, 1]),
        )

    for m in range(2):
        for cp in raw_copies(m):
            cp.start()
    pp_copy = pltpu.make_async_copy(pp_hbm, pp, pp_sem)
    pp_copy.start()

    pvr[...] = jnp.zeros_like(pvr)
    barrier = pltpu.get_barrier_semaphore()
    for who in (to_l, to_r, sib, *dims, *far):
        pl.semaphore_signal(barrier, inc=1, device_id=who, device_id_type=MESH)

    zrow = jnp.zeros((2, SLOTS, 3, 64, 128), BF)
    for buf in (rown, rfor):
        for start in (0, 256):
            buf[:, :, :, pl.ds(start, 64), :] = zrow

    def l_copy(p, m):
        at = pl.ds(NS * m, NS)
        return pltpu.make_async_remote_copy(
            src_ref=lown.at[p, at], dst_ref=lfor.at[p, at], send_sem=l_ss.at[p, m], recv_sem=l_rs.at[p, m],
            device_id=to_l, device_id_type=MESH)

    def r_copy(p, m):
        at = pl.ds(NS * m, NS)
        rows = pl.ds(64, W)
        return pltpu.make_async_remote_copy(
            src_ref=rown.at[p, at, :, rows, :], dst_ref=rfor.at[p, at, :, rows, :],
            send_sem=r_ss.at[p, m], recv_sem=r_rs.at[p, m], device_id=to_r, device_id_type=MESH)

    def pack(m):
        buf = m % 2

        def one(k, carry):
            s = k // 2
            p = k % 2
            slot = NS * m + s
            row = iota((W, 128), 0)
            live = slot < count[0]
            keep = []
            for par in range(2):
                size = jnp.where(live, lsize[x * 4 + 2 * p + par], 0)
                keep.append(one_hot(row < size))
            ev = raw[buf, 0, s, 2 * p]
            od = raw[buf, 0, s, 2 * p + 1]
            lown[p, slot, 0] = ev[:, :128] * keep[0]
            lown[p, slot, 1] = od[:, :128] * keep[1]
            lown[p, slot, 2] = jnp.concatenate(
                [ev[:, 128:] * keep[0][:, :64], od[:, 128:] * keep[1][:, :64]], axis=1)
            ev = raw[buf, 1, s, 2 * p]
            od = raw[buf, 1, s, 2 * p + 1]
            rows = pl.ds(64, W)
            rown[p, slot, 0, rows, :] = ev[:, :128]
            rown[p, slot, 1, rows, :] = od[:, :128]
            rown[p, slot, 2, rows, :] = jnp.concatenate([ev[:, 128:], od[:, 128:]], axis=1)
            return carry

        lax.fori_loop(0, 2 * NS, one, 0)

    for m in range(NC):
        for cp in raw_copies(m):
            cp.wait()
        pack(m)
        if m == 0:
            pl.semaphore_wait(barrier, 10)
        if m + 2 < NC:
            for cp in raw_copies(m + 2):
                cp.start()
        l_copy(0, m).start()
        r_copy(0, m).start()
    for m in range(NC):
        l_copy(1, m).start()
        r_copy(1, m).start()

    def clear(k, carry):
        for g in range(2):
            for q in range(4):
                acc[g, q, k // 2, pl.ds(pl.multiple_of((k % 2) * W, W), W), :] = jnp.zeros((W, 384), F32)
        return carry

    lax.fori_loop(0, 4, clear, 0)
    pp_copy.wait()

    def product(m, r, lefts):
        rsrc = rown if r < 2 else rfor
        slots = pl.ds(NS * m, NS)
        for par in range(2):
            j = 2 * r + par
            for n, (h, l) in enumerate(lefts):
                lsrc = lown if h == 0 else lfor
                tail = lsrc[l, slots, 2].reshape(NS * W, 128)
                for pa in range(2):
                    lhs = jnp.concatenate([lsrc[l, slots, pa].reshape(NS * W, 128), tail], axis=1)
                    img = jnp.dot(lhs, pp[j, pl.ds((h * 4 + 2 * l + pa) * 256, 256), :],
                                  preferred_element_type=F32).astype(BF)
                    for s in range(NS):
                        li[pl.ds((2 * n + pa) * W, W), pl.ds(s * 256, 256)] = img[s * W:(s + 1) * W]
            rows = pl.ds(64 - 64 * par, 256)
            rhs = jnp.concatenate(
                [rsrc[r % 2, NS * m + s, k, rows, :] for s in range(NS) for k in (par, 2)], axis=1)
            lanes = pl.ds(128 * par, 256)
            for n, (h, l) in enumerate(lefts):
                g, q, cell = PLACE[(h, l, r)]
                res = lax.dot_general(li[pl.ds(2 * n * W, 2 * W), :], rhs, (((1,), (1,)), ((), ())),
                                      preferred_element_type=F32)
                for pa in range(2):
                    acc[g, q, pa, pl.ds(cell * W, W), lanes] += res[pa * W:(pa + 1) * W]

    def arrive(p, m):
        l_copy(p, m).wait()
        r_copy(p, m).wait()

    def d_copy(g, qi):
        return pltpu.make_async_remote_copy(
            src_ref=acc.at[g, qi, 1 - c], dst_ref=drecv.at[g, qi],
            send_sem=d_ss.at[g, qi], recv_sem=d_rs.at[g, qi], device_id=sib, device_id_type=MESH)

    rsb = (rs0, rs1, rs2, rs3)

    def rs_copy(g, qi, s):
        d = (qi + s) % 4
        if s < 3:
            rows = STEP[s]
            first = offs[qi][s] + (1 - bits[d]) * rows
        else:
            rows, first = 48, offs[qi][3]
        return pltpu.make_async_remote_copy(
            src_ref=acc.at[g, qi, c, pl.ds(pl.multiple_of(first, 16), rows), :],
            dst_ref=rsb[s].at[g, qi], send_sem=rs_ss.at[g, qi, s], recv_sem=rs_rs.at[g, qi, s],
            device_id=dims[d], device_id_type=MESH)

    def add_rows(g, qi, first, src, src_first, rows):
        def step(k, carry):
            at = pl.ds(pl.multiple_of(first + k * 48, 16), 48)
            acc[g, qi, c, at, :] += src[pl.ds(pl.multiple_of(src_first + k * 48, 16), 48), :]
            return carry

        lax.fori_loop(0, rows // 48, step, 0)

    def core_sum(g):
        for qi in range(4):
            d_copy(g, qi).wait_recv()
            there = (1 - bits[qi]) * 192
            here = bits[qi] * 192
            add_rows(g, qi, there, drecv.at[g, qi], there, 192)
            rs_copy(g, qi, 0).start()
            add_rows(g, qi, here, drecv.at[g, qi], here, 192)

    def x_copy(g, qi):
        return pltpu.make_async_remote_copy(
            src_ref=acc.at[g, qi, c, pl.ds(pl.multiple_of(offs[qi][3], 16), 48), :], dst_ref=xrecv.at[g, qi],
            send_sem=x_ss.at[g, qi], recv_sem=x_rs.at[g, qi], device_id=to_l, device_id_type=MESH)

    def reduce_step(g, s):
        for qi in range(4):
            rs_copy(g, qi, s).wait_recv()
            if s == 3:
                rs_copy(g, qi, 3).wait_send()
                add_rows(g, qi, offs[qi][3], rs3.at[g, qi], 0, 48)
                if CELLS[g][qi][0] == 1:
                    x_copy(g, qi).start()
            else:
                add_rows(g, qi, offs[qi][s + 1], rsb[s].at[g, qi], 0, STEP[s])
                rs_copy(g, qi, s + 1).start()

    def rows_at(g, qi, first, rows, core):
        n = first // W
        l, r = cell_at(g, qi, n)
        at = (2 * l + core) * W + first - n * W
        return CELLS[g][qi][0] * 4 + r, pl.ds(pl.multiple_of(at, 16), rows)

    def ag_copy(g, qi, s, mine):
        d = (qi + s) % 4
        first = offs[qi][s + 1] if mine else offs[qi][s] + (1 - bits[d]) * STEP[s]
        k, at = rows_at(g, qi, first, STEP[s], c)
        return pltpu.make_async_remote_copy(
            src_ref=slabs.at[k, at, :], dst_ref=slabs.at[k, at, :],
            send_sem=ag_ss.at[g, qi, s], recv_sem=ag_rs.at[g, qi, s],
            device_id=dims[d], device_id_type=MESH)

    def fw_copy(g, qi, s, core):
        if s == 3:
            first, rows = offs[qi][3], 48
        else:
            first, rows = offs[qi][s] + (1 - bits[(qi + s) % 4]) * STEP[s], STEP[s]
        k, at = rows_at(g, qi, first, rows, core)
        return pltpu.make_async_remote_copy(
            src_ref=slabs.at[k, at, :], dst_ref=slabs.at[k, at, :],
            send_sem=fw_ss.at[g, qi, s], recv_sem=fw_rs.at[g, qi, s],
            device_id=sib, device_id_type=MESH)

    sums = [jnp.zeros((1, 1), F32), jnp.zeros((1, 1), F32)]

    def finish(g, h):
        for qi in range(4):
            if CELLS[g][qi][0] != h:
                continue
            off = offs[qi][3]
            if h == 0:
                part = acc[g, qi, c, pl.ds(pl.multiple_of(off, 16), 48), :]
            else:
                x_copy(g, qi).wait_recv()
                part = xrecv[g, qi]
            full = part + diag[g * 4 + qi + jnp.minimum(lsize[0], 0)]
            k, at = rows_at(g, qi, off, 48, c)
            slabs[k, at, :] = full.astype(BF)
            ag_copy(g, qi, 2, True).start()
            fw_copy(g, qi, 3, c).start()
            weight = (1 - bits[(qi + 3) % 4]).astype(F32)
            for k in range(2):
                sums[k] = sums[k] + weight * jnp.sum(full * subp[g * 4 + qi, k], keepdims=True)

    def gather_step(g, s, h=None):
        for qi in range(4):
            if h is not None and CELLS[g][qi][0] != h:
                continue
            ag_copy(g, qi, s, False).wait_recv()
            if s > 0:
                ag_copy(g, qi, s - 1, True).start()
            fw_copy(g, qi, s, c).start()

    def step0(m, carry):
        for r in range(2):
            product(m, r, ((0, 0), (0, 1)))
        return carry

    lax.fori_loop(0, NC, step0, 0)

    def step1(m, carry):
        arrive(0, m)
        for r in range(2):
            product(m, r, ((1, 0),))
        product(m, 2, ((0, 0), (0, 1), (1, 0)))
        return carry

    lax.fori_loop(0, NC, step1, 0)
    for qi in range(4):
        d_copy(0, qi).start()

    def first_half(m):
        arrive(1, m)
        for r in range(3):
            product(m, r, ((1, 1),))

    def second_half(m):
        product(m, 3, ((0, 0), (0, 1), (1, 0), (1, 1)))

    first_half(0)
    core_sum(0)
    second_half(0)
    first_half(1)
    reduce_step(0, 0)
    second_half(1)
    reduce_step(0, 1)
    first_half(2)
    reduce_step(0, 2)
    second_half(2)
    reduce_step(0, 3)
    finish(0, 0)
    first_half(3)
    for qi in (1, 2):
        d_copy(1, qi).start()
    second_half(3)
    for qi in (0, 3):
        d_copy(1, qi).start()
    finish(0, 1)
    gather_step(0, 2)
    core_sum(1)
    gather_step(0, 1)
    reduce_step(1, 0)
    gather_step(0, 0)
    reduce_step(1, 1)
    reduce_step(1, 2)
    reduce_step(1, 3)
    finish(1, 0)
    finish(1, 1)

    lane = iota((8, 128), 1)
    pvs[0] = jnp.where(lane == 0, sums[0], jnp.where(lane == 1, sums[1], F32(0)))
    rounds = (
        (c, ((sib, 1 - c),)),
        (y, ((dims[0], y_a), (dims[2], 3 - y), (far[0], y_c))),
        (z, ((dims[1], z_a), (dims[3], 3 - z), (far[1], z_c))),
        (x, ((to_l, x_l), (to_r, x_r), (far[2], x_c))),
    )

    def pv_copy(n, i, slot):
        return pltpu.make_async_remote_copy(
            src_ref=pvs.at[n], dst_ref=pvr.at[n, slot], send_sem=pv_ss.at[n, i], recv_sem=pv_rs.at[n, slot],
            device_id=rounds[n][1][i][0], device_id_type=MESH)

    def pv_send(n):
        me, others = rounds[n]
        for i in range(len(others)):
            pv_copy(n, i, me).start()
        pvr[n, me] = pvs[n]

    def pv_sum(n):
        me, others = rounds[n]
        for i, (who, slot) in enumerate(others):
            pv_copy(n, i, slot).wait_recv()
        pvs[n + 1] = (pvr[n, 0] + pvr[n, 1]) + (pvr[n, 2] + pvr[n, 3])

    def o_copy(k, core):
        rows = tuple(pl.ds((2 * l + core) * W, W) for l in range(2))
        return [pltpu.make_async_copy(slabs.at[k, at, :], out_hbm.at[k, at, :], out_sem.at[k, core, l])
                for l, at in enumerate(rows)]

    pv_send(0)
    for n, s in enumerate((2, 1, 0)):
        gather_step(1, s)
        pv_sum(n)
        pv_send(n + 1)
    for k in range(8):
        for cp in o_copy(k, c):
            cp.start()
    for g in range(2):
        for s in (3, 2, 1, 0):
            for qi in range(4):
                fw_copy(g, qi, s, 1 - c).wait_recv()
    for k in range(8):
        for cp in o_copy(k, 1 - c):
            cp.start()
    pv_sum(3)
    proj_out[...] = pvs[4]
    for g in range(2):
        for qi in range(4):
            d_copy(g, qi).wait_send()
            for s in range(3):
                rs_copy(g, qi, s).wait_send()
                ag_copy(g, qi, s, True).wait_send()
            for s in range(4):
                fw_copy(g, qi, s, c).wait_send()
            if CELLS[g][qi][0] == 1:
                x_copy(g, qi).wait_send()
    for n in range(4):
        for i in range(len(rounds[n][1])):
            pv_copy(n, i, rounds[n][0]).wait_send()
    for k in range(8):
        for core in (c, 1 - c):
            for cp in o_copy(k, core):
                cp.wait()


def compact_body(rstart, rsize, src, out):
    x = lax.axis_index("site")
    k = pl.program_id(0)
    x_l = x + 1 - 2 * (x % 2)

    @pl.when(k == 0)
    def _():
        out[...] = jnp.zeros_like(out)

    xt = jnp.where(k // 4 == 0, x, x_l)
    site = xt + ((k // 2) % 2) * (3 - 2 * xt)
    q = site * 4 + 2 * (k % 2)
    start = rstart[q]
    base = pl.multiple_of(jnp.minimum((start // 128) * 128, BOND - 512), 128)
    j = iota((384, 512), 0)
    odd = j >= W
    idx = jnp.where(odd, j - W, j)
    size = jnp.where(odd, rsize[q + 1], rsize[q])
    first = jnp.where(odd, rstart[q + 1], start) - base
    hot = one_hot((idx < size) & (iota((384, 512), 1) == idx + first))
    out[:, pl.ds(base, 512)] += jnp.dot(src[0], hot, preferred_element_type=F32).astype(BF)


def sector_tables(sector_ids, sectors):
    labels = jnp.arange(sectors, dtype=jnp.int32)
    starts = jnp.sum((sector_ids[None, :] < labels[:, None]).astype(jnp.int32), axis=1)
    sizes = jnp.sum((sector_ids[None, :] == labels[:, None]).astype(jnp.int32), axis=1)
    return starts, sizes


def local(wavefunction, left_blocks, right_blocks, left_sector, right_sector, term_count,
          left_energy, right_energy, subspace):
    lstart, lsize = sector_tables(left_sector, 16)
    rstart, rsize = sector_tables(right_sector, 16)
    smem = pl.BlockSpec(memory_space=pltpu.SMEM)
    vmem = pl.BlockSpec(memory_space=pltpu.VMEM)
    hbm = pl.BlockSpec(memory_space=pl.ANY)
    dma = pltpu.SemaphoreType.DMA
    big = pltpu.CompilerParams(vmem_limit_bytes=67043328)
    pp, diag, subp = pl.pallas_call(
        prep_body,
        out_shape=(jax.ShapeDtypeStruct((8, 2048, 256), BF), jax.ShapeDtypeStruct((8, 48, 384), F32),
                   jax.ShapeDtypeStruct((8, 2, 48, 384), F32)),
        in_specs=[smem] * 4 + [vmem] * 3 + [hbm],
        out_specs=(hbm, vmem, vmem),
        scratch_shapes=[
            pltpu.VMEM((2048, BOND), BF),
            pltpu.VMEM((8, 2048, 256), BF),
            pltpu.VMEM((8, 160, BOND), BF),
            dma((8, 2)), dma((8,)),
        ],
        compiler_params=big,
        name="prepare",
    )(lstart, lsize, rstart, rsize, wavefunction,
      left_energy.reshape(1, BOND), right_energy.reshape(1, BOND), subspace)
    slabs, proj = pl.pallas_call(
        body,
        out_shape=(jax.ShapeDtypeStruct((8, 768, 384), BF), jax.ShapeDtypeStruct((8, 128), F32)),
        in_specs=[smem] * 2 + [hbm] * 3 + [vmem] * 2,
        out_specs=(hbm, vmem),
        scratch_shapes=[
            pltpu.VMEM((8, 768, 384), BF),
            pltpu.VMEM((8, 2048, 256), BF),
            pltpu.VMEM((2, 2, NS, 4, W, W), BF),
            pltpu.VMEM((2, SLOTS, 3, W, 128), BF),
            pltpu.VMEM((2, SLOTS, 3, W, 128), BF),
            pltpu.VMEM((2, SLOTS, 3, 320, 128), BF),
            pltpu.VMEM((2, SLOTS, 3, 320, 128), BF),
            pltpu.VMEM((1536, NS * 256), BF),
            pltpu.VMEM((2, 4, 2, 384, 384), F32),
            pltpu.VMEM((2, 4, 384, 384), F32),
            pltpu.VMEM((2, 4, 192, 384), F32),
            pltpu.VMEM((2, 4, 96, 384), F32),
            pltpu.VMEM((2, 4, 48, 384), F32),
            pltpu.VMEM((2, 4, 48, 384), F32),
            pltpu.VMEM((2, 4, 48, 384), F32),
            pltpu.VMEM((5, 8, 128), F32),
            pltpu.VMEM((4, 4, 8, 128), F32),
            dma((2, 2)), dma, dma((8, 2, 2)),
            dma((2, NC)), dma((2, NC)), dma((2, NC)), dma((2, NC)),
            dma((2, 4)), dma((2, 4)), dma((2, 4, 4)), dma((2, 4, 4)), dma((2, 4)), dma((2, 4)),
            dma((2, 4, 3)), dma((2, 4, 3)), dma((2, 4, 4)), dma((2, 4, 4)), dma((4, 3)), dma((4, 4)),
        ],
        compiler_params=pltpu.CompilerParams(
            collective_id=0, has_side_effects=True, vmem_limit_bytes=67043328),
        name="exchange",
    )(lsize, term_count, pp, left_blocks, right_blocks, diag, subp)
    sigma = pl.pallas_call(
        compact_body,
        grid=(8,),
        out_shape=jax.ShapeDtypeStruct((768, BOND), BF),
        in_specs=[smem, smem, pl.BlockSpec((1, 768, 384), lambda k: (k, 0, 0))],
        out_specs=pl.BlockSpec((768, BOND), lambda k: (0, 0)),
        name="compact",
    )(rstart, rsize, slabs)
    return sigma.reshape(4, W, BOND), proj[0, :2]


def solution(mesh):
    in_specs = (P(), P("ops", "site", None, None), P("ops", "site", None, None), P(), P(), P("ops"),
                P(), P(), P(None, "site", None, None))
    out_specs = (P("site", None, None), P())
    return jax.shard_map(local, mesh=mesh, in_specs=in_specs, out_specs=out_specs, check_vma=False)
```

```python
import jax
import jax.numpy as jnp
from jax import lax
from jax.experimental import pallas as pl
from jax.experimental.pallas import tpu as pltpu
from jax.sharding import PartitionSpec as P

W = 192
SLOTS = 8
NS = 2
NC = SLOTS // NS
BOND = 2048
BF = jnp.bfloat16
F32 = jnp.float32
MESH = pl.DeviceIdType.MESH


def iota(shape, dim):
    return lax.broadcasted_iota(jnp.int32, shape, dim)


def one_hot(mask):
    return jnp.where(mask, F32(1), F32(0)).astype(BF)


def packed_index(pos, parity):
    tail = pos - 64 * parity
    idx = jnp.where(pos < 128, pos, tail)
    ok = (pos < 128) | ((tail >= 128) & (tail < W))
    return idx, ok


CELLS = (
    ((0, ((0, 0), (0, 1))), (0, ((1, 0), (1, 1))), (0, ((0, 2), (1, 2))), (1, ((0, 0), (0, 1)))),
    ((0, ((0, 3), (1, 3))), (1, ((1, 0), (1, 1))), (1, ((0, 2), (1, 2))), (1, ((0, 3), (1, 3)))),
)
PLACE = {
    (h, l, r): (g, q, n)
    for g in range(2) for q, (h, pair) in enumerate(CELLS[g]) for n, (l, r) in enumerate(pair)
}
STEP = (192, 96, 48)


def piece_offsets(bits):
    offs = []
    for qi in range(4):
        off = [0]
        for s in range(3):
            off.append(off[-1] + bits[(qi + s) % 4] * STEP[s])
        offs.append(off)
    return offs


def cell_at(g, qi, n):
    (l0, r0), (l1, r1) = CELLS[g][qi][1]
    return l0 + n * (l1 - l0), r0 + n * (r1 - r0)


def label_bits(y, z):
    return (((y + 1) // 2) % 2, ((z + 1) // 2) % 2, y // 2, z // 2)


def body(
    lstart, lsize, rstart, rsize, count,
    psi_hbm, left_hbm, right_hbm, lenergy, renergy, sub_hbm,
    out_hbm, proj_out,
    psi_v, gath, pp, raw, lall, rb, li, acc, subv, diag, subp,
    rs0, rs1, rs2, rs3, xrecv, pvs, pvr,
    raw_sem, psi_sem, sub_sem, out_sem,
    l_ss, l_rs, ls_ss, ls_rs, r_ss, r_rs, ro_ss, ro_rs, rf_ss, rf_rs, rs_ss, rs_rs, x_ss, x_rs,
    ag_ss, ag_rs, fw_ss, fw_rs, pv_ss, pv_rs,
):
    x = lax.axis_index("site")
    o = lax.axis_index("ops")
    c = o % 2
    y = (o // 2) % 4
    z = o // 8
    x_l = x + 1 - 2 * (x % 2)
    x_r = 3 - x
    to_l = {"site": x_l}
    to_r = {"site": x_r}
    sib = {"ops": o + 1 - 2 * c}
    to_ls = {"ops": o + 1 - 2 * c, "site": x_l}
    y_a = y + 1 - 2 * (y % 2)
    z_a = z + 1 - 2 * (z % 2)
    y_c = 3 - y_a
    z_c = 3 - z_a
    x_c = 3 - x_l
    dims = (
        {"ops": o + 2 * (y_a - y)},
        {"ops": o + 8 * (z_a - z)},
        {"ops": o + 2 * (3 - 2 * y)},
        {"ops": o + 8 * (3 - 2 * z)},
    )
    far = ({"ops": o + 2 * (y_c - y)}, {"ops": o + 8 * (z_c - z)}, {"site": x_c})
    bits = label_bits(y, z)
    offs = piece_offsets(bits)
    data = pl.ds(64, W)

    def raw_copies(m):
        buf = m % 2
        return (
            pltpu.make_async_copy(left_hbm.at[pl.ds(NS * m, NS)], raw.at[buf, 0], raw_sem.at[buf, 0]),
            pltpu.make_async_copy(right_hbm.at[pl.ds(NS * m, NS)], raw.at[buf, 1], raw_sem.at[buf, 1]),
        )

    for m in range(2):
        for cp in raw_copies(m):
            cp.start()
    psi_copy = pltpu.make_async_copy(psi_hbm, psi_v, psi_sem)
    psi_copy.start()

    pvr[...] = jnp.zeros_like(pvr)
    barrier = pltpu.get_barrier_semaphore()
    for who in (to_l, to_r, sib, to_ls, *dims, *far):
        pl.semaphore_signal(barrier, inc=1, device_id=who, device_id_type=MESH)

    def l_copy(ph, m, w):
        at = pl.ds(NS * m, NS)
        tiles = pl.ds(0, 2) if ph == 0 else pl.ds(2, 1)
        return pltpu.make_async_remote_copy(
            src_ref=lall.at[c if w == 0 else 1 - c, at, tiles], dst_ref=lall.at[3 + w, at, tiles],
            send_sem=l_ss.at[ph, m, w], recv_sem=l_rs.at[ph, m, w],
            device_id=to_l if w == 0 else to_ls, device_id_type=MESH)

    def ls_copy(m):
        at = pl.ds(NS * m, NS)
        return pltpu.make_async_remote_copy(
            src_ref=lall.at[1 - c, at], dst_ref=lall.at[2, at], send_sem=ls_ss.at[m], recv_sem=ls_rs.at[m],
            device_id=sib, device_id_type=MESH)

    def r_copy(p, m):
        at = pl.ds(NS * m, NS)
        return pltpu.make_async_remote_copy(
            src_ref=rb.at[0, p, at, :, data, :], dst_ref=rb.at[2, p, at, :, data, :],
            send_sem=r_ss.at[p, m], recv_sem=r_rs.at[p, m], device_id=to_r, device_id_type=MESH)

    def ro_copy(m):
        at = pl.ds(NS * m, NS)
        return pltpu.make_async_remote_copy(
            src_ref=rb.at[0, :, at, :, data, :], dst_ref=rb.at[1, :, at, :, data, :],
            send_sem=ro_ss.at[m], recv_sem=ro_rs.at[m], device_id=sib, device_id_type=MESH)

    def rf_copy(p, m):
        at = pl.ds(NS * m, NS)
        return pltpu.make_async_remote_copy(
            src_ref=rb.at[2, p, at, :, data, :], dst_ref=rb.at[3, p, at, :, data, :],
            send_sem=rf_ss.at[p, m], recv_sem=rf_rs.at[p, m], device_id=sib, device_id_type=MESH)

    def pack(m):
        buf = m % 2

        def one(k, carry):
            s = k // 2
            p = k % 2
            slot = NS * m + s
            row = iota((W, 128), 0)
            live = slot < count[0]
            keep = []
            for n in range(2):
                size = jnp.where(live, lsize[x * 4 + 2 * n + p], 0)
                keep.append(one_hot(row < size))
            ev = raw[buf, 0, s, p]
            od = raw[buf, 0, s, 2 + p]
            lall[p, slot, 0] = ev[:, :128] * keep[0]
            lall[p, slot, 2] = od[:, :128] * keep[1]
            lall[p, slot, 1] = jnp.concatenate(
                [ev[:, 128:] * keep[0][:, :64], od[:, 128:] * keep[1][:, :64]], axis=1)
            ev = raw[buf, 1, s, 2 * p]
            od = raw[buf, 1, s, 2 * p + 1]
            rb[0, p, slot, 0, data, :] = ev[:, :128]
            rb[0, p, slot, 1, data, :] = od[:, :128]
            rb[0, p, slot, 2, data, :] = jnp.concatenate([ev[:, 128:], od[:, 128:]], axis=1)
            return carry

        lax.fori_loop(0, 2 * NS, one, 0)

    for m in range(NC):
        for cp in raw_copies(m):
            cp.wait()
        pack(m)
        if m == 0:
            pl.semaphore_wait(barrier, 11)
        if m + 2 < NC:
            for cp in raw_copies(m + 2):
                cp.start()
        for w in range(2):
            l_copy(0, m, w).start()
        r_copy(0, m).start()
        ls_copy(m).start()
        ro_copy(m).start()
    for m in range(NC):
        for w in range(2):
            l_copy(1, m, w).start()
        r_copy(1, m).start()

    def piece(g, qi):
        off = offs[qi][3]
        n = off // W
        l, r = cell_at(g, qi, n)
        return 2 * l + c, off - n * W, r

    def sub_copy(g, qi, k):
        i, a0, r = piece(g, qi)
        return pltpu.make_async_copy(
            sub_hbm.at[k, i, pl.ds(pl.multiple_of(a0, 16), 48), :],
            subv.at[g * 4 + qi, k], sub_sem.at[g * 4 + qi, k])

    for g in range(2):
        for qi in range(4):
            for k in range(2):
                sub_copy(g, qi, k).start()

    zrow = jnp.zeros((SLOTS, 3, 64, 128), BF)

    def clear(k, carry):
        for start in (0, 256):
            rb[k // 2, k % 2, :, :, pl.ds(start, 64), :] = zrow
        acc[k // 4, k % 4] = jnp.zeros((384, 384), F32)
        return carry

    lax.fori_loop(0, 8, clear, 0)

    psi_copy.wait()

    def row_hot(q, first, rows, half):
        rs = lstart[q]
        t0 = jnp.minimum(rs // 16, BOND // 16 - 16)
        pos = iota((rows, 256), 0) + first
        if half is None:
            idx, ok = pos, pos < W
        else:
            idx, ok = packed_index(pos, half)
        ok = ok & (idx < lsize[q])
        return t0, one_hot(ok & (iota((rows, 256), 1) == idx + (rs - t0 * 16)))

    def put_rows(at, rows, t0, hot):
        for n in range(4):
            win = jnp.concatenate([psi_v[t0 + k, :, pl.ds(n * 512, 512)] for k in range(16)], axis=0)
            got = jnp.dot(hot, win, preferred_element_type=F32).astype(BF)
            for k in range(4):
                gath[n * 4 + k, pl.ds(at, rows), :] = got[:, k * 128:(k + 1) * 128]

    def rows_of(i, carry):
        q = jnp.where(i < 2, x, x_l) * 4 + 2 * (i % 2) + c
        t0, hot = row_hot(q, 0, 256, i % 2)
        put_rows(pl.multiple_of(i * 256, 256), 256, t0, hot)
        return carry

    lax.fori_loop(0, 4, rows_of, 0)

    def cols_of(j, carry):
        q = jnp.where(j < 4, x * 4 + j, x_r * 4 + j - 4)
        cs = rstart[q]
        ct = jnp.minimum(cs // 128, BOND // 128 - 3)
        idx, ok = packed_index(iota((384, 256), 1), q % 2)
        ok = ok & (idx < rsize[q])
        hot = one_hot(ok & (iota((384, 256), 0) == idx + (cs - ct * 128)))
        for m in range(2):
            win = jnp.concatenate([gath[ct + k, pl.ds(m * 512, 512), :] for k in range(3)], axis=1)
            pp[j, pl.ds(m * 512, 512), :] = jnp.dot(win, hot, preferred_element_type=F32).astype(BF)
        return carry

    lax.fori_loop(0, 8, cols_of, 0)

    def own_rows():
        re = renergy[...]
        hi = re.astype(BF)
        rem = re - hi.astype(F32)
        mid = rem.astype(BF)
        low = (rem - mid.astype(F32)).astype(BF)
        rows16 = iota((16, BOND), 0)
        er3 = jnp.where(rows16 == 0, hi.astype(F32),
                        jnp.where(rows16 == 1, mid.astype(F32),
                                  jnp.where(rows16 == 2, low.astype(F32), F32(0)))).astype(BF)
        for t in range(16):
            for qi in range(4):
                gath[t, pl.ds(qi * 160 + 144, 16), :] = er3[:, t * 128:(t + 1) * 128]
        for g in range(2):
            for qi in range(4):
                n8 = g * 4 + qi
                at = qi * 160
                i, a0, r = piece(g, qi)
                q = x * 4 + i
                t0, hot = row_hot(q, a0, 48, None)
                put_rows(at, 48, t0, hot)
                for k in range(2):
                    sub_copy(g, qi, k).wait()
                    for t in range(16):
                        gath[t, pl.ds(at + 48 + 48 * k, 48), :] = subv[n8, k, :, pl.ds(t * 128, 128)]
                xt = x if CELLS[g][qi][0] == 0 else x_l
                site = xt + (r // 2) * (3 - 2 * xt)
                total = None
                for par in range(2):
                    qr = site * 4 + 2 * (r % 2) + par
                    cs = rstart[qr]
                    ct = jnp.minimum(cs // 128, BOND // 128 - 3)
                    j = iota((384, 384), 1) - W * par
                    hot2 = one_hot((j >= 0) & (j < W) & (j < rsize[qr])
                                   & (iota((384, 384), 0) == j + (cs - ct * 128)))
                    win = jnp.concatenate([gath[ct + k, pl.ds(at, 160), :] for k in range(3)], axis=1)
                    part = jnp.dot(win, hot2, preferred_element_type=F32)
                    total = part if total is None else total + part
                lt = jnp.minimum(lstart[q] // 128, BOND // 128 - 3)
                shift = lstart[q] - lt * 128 + a0
                pick = iota((48, 384), 1) == iota((48, 384), 0) + shift
                lrow = jnp.concatenate([lenergy[lt + k] for k in range(3)], axis=1)
                el = jnp.sum(jnp.where(pick, lrow, F32(0)), axis=1, keepdims=True)
                er = total[144:145] + total[145:146] + total[146:147]
                diag[n8] = (el + er) * total[:48]
                subp[n8, 0] = total[48:96]
                subp[n8, 1] = total[96:144]

    left_at = {(0, 0): c, (0, 1): 2, (1, 0): 3, (1, 1): 4}

    def product(m, w, r, lefts):
        slots = pl.ds(NS * m, NS)
        side = (0 if r < 2 else 2) + w
        for par in range(2):
            j = 2 * r + par
            for n, (h, l) in enumerate(lefts):
                src = left_at[(h, w)]
                lhs = jnp.concatenate([lall[src, slots, 2 * l].reshape(NS * W, 128),
                                       lall[src, slots, 1].reshape(NS * W, 128)], axis=1)
                img = jnp.dot(lhs, pp[j, pl.ds((2 * h + l) * 256, 256), :],
                              preferred_element_type=F32).astype(BF)
                for s in range(NS):
                    li[pl.ds(n * W, W), pl.ds(s * 256, 256)] = img[s * W:(s + 1) * W]
            rows = pl.ds(64 - 64 * par, 256)
            rhs = jnp.concatenate(
                [rb[side, r % 2, NS * m + s, k, rows, :] for s in range(NS) for k in (par, 2)], axis=1)
            lanes = pl.ds(128 * par, 256)
            res = lax.dot_general(li[pl.ds(0, len(lefts) * W), :], rhs, (((1,), (1,)), ((), ())),
                                  preferred_element_type=F32)
            for n, (h, l) in enumerate(lefts):
                g, q, cell = PLACE[(h, l, r)]
                acc[g, q, pl.ds(cell * W, W), lanes] += res[n * W:(n + 1) * W]

    def arrive(p, m):
        r_copy(p, m).wait()
        rf_copy(p, m).start()
        for w in range(2):
            l_copy(p, m, w).wait()

    rsb = (rs0, rs1, rs2, rs3)

    def rs_copy(g, qi, s):
        d = (qi + s) % 4
        if s < 3:
            rows = STEP[s]
            first = offs[qi][s] + (1 - bits[d]) * rows
        else:
            rows, first = 48, offs[qi][3]
        return pltpu.make_async_remote_copy(
            src_ref=acc.at[g, qi, pl.ds(pl.multiple_of(first, 16), rows), :],
            dst_ref=rsb[s].at[g, qi], send_sem=rs_ss.at[g, qi, s], recv_sem=rs_rs.at[g, qi, s],
            device_id=dims[d], device_id_type=MESH)

    def add_rows(g, qi, first, src, src_first, rows):
        def step(k, carry):
            at = pl.ds(pl.multiple_of(first + k * 48, 16), 48)
            acc[g, qi, at, :] += src[pl.ds(pl.multiple_of(src_first + k * 48, 16), 48), :]
            return carry

        lax.fori_loop(0, rows // 48, step, 0)

    def x_copy(g, qi):
        return pltpu.make_async_remote_copy(
            src_ref=acc.at[g, qi, pl.ds(pl.multiple_of(offs[qi][3], 16), 48), :], dst_ref=xrecv.at[g, qi],
            send_sem=x_ss.at[g, qi], recv_sem=x_rs.at[g, qi], device_id=to_l, device_id_type=MESH)

    def reduce_step(g, s):
        for qi in range(4):
            rs_copy(g, qi, s).wait_recv()
            if s == 3:
                rs_copy(g, qi, 3).wait_send()
                add_rows(g, qi, offs[qi][3], rs3.at[g, qi], 0, 48)
                if CELLS[g][qi][0] == 1:
                    x_copy(g, qi).start()
            else:
                add_rows(g, qi, offs[qi][s + 1], rsb[s].at[g, qi], 0, STEP[s])
                rs_copy(g, qi, s + 1).start()

    def rows_at(g, qi, first, rows, core):
        n = first // W
        l, r = cell_at(g, qi, n)
        tile = CELLS[g][qi][0] * 48 + (2 * l + core) * 12 + (first - n * W) // 16
        return pl.ds(tile, rows // 16), pl.ds(pl.multiple_of(r * 384, 128), 384)

    def ag_copy(g, qi, s, mine):
        d = (qi + s) % 4
        first = offs[qi][s + 1] if mine else offs[qi][s] + (1 - bits[d]) * STEP[s]
        at, lanes = rows_at(g, qi, first, STEP[s], c)
        return pltpu.make_async_remote_copy(
            src_ref=psi_v.at[at, :, lanes], dst_ref=psi_v.at[at, :, lanes],
            send_sem=ag_ss.at[g, qi, s], recv_sem=ag_rs.at[g, qi, s],
            device_id=dims[d], device_id_type=MESH)

    def fw_copy(g, qi, s, core):
        if s == 3:
            first, rows = offs[qi][3], 48
        else:
            first, rows = offs[qi][s] + (1 - bits[(qi + s) % 4]) * STEP[s], STEP[s]
        at, lanes = rows_at(g, qi, first, rows, core)
        return pltpu.make_async_remote_copy(
            src_ref=psi_v.at[at, :, lanes], dst_ref=psi_v.at[at, :, lanes],
            send_sem=fw_ss.at[g, qi, s], recv_sem=fw_rs.at[g, qi, s],
            device_id=sib, device_id_type=MESH)

    sums = [jnp.zeros((1, 1), F32), jnp.zeros((1, 1), F32)]

    def finish(g, h):
        for qi in range(4):
            if CELLS[g][qi][0] != h:
                continue
            off = offs[qi][3]
            if h == 0:
                part = acc[g, qi, pl.ds(pl.multiple_of(off, 16), 48), :]
            else:
                x_copy(g, qi).wait_recv()
                part = xrecv[g, qi]
            full = part + diag[g * 4 + qi]
            at, lanes = rows_at(g, qi, off, 48, c)
            psi_v[at, :, lanes] = full.astype(BF).reshape(3, 16, 384)
            ag_copy(g, qi, 2, True).start()
            fw_copy(g, qi, 3, c).start()
            weight = (1 - bits[(qi + 3) % 4]).astype(F32)
            for k in range(2):
                sums[k] = sums[k] + weight * jnp.sum(full * subp[g * 4 + qi, k], keepdims=True)

    def gather_step(g, s, h=None):
        for qi in range(4):
            if h is not None and CELLS[g][qi][0] != h:
                continue
            ag_copy(g, qi, s, False).wait_recv()
            if s > 0:
                ag_copy(g, qi, s - 1, True).start()
            fw_copy(g, qi, s, c).start()

    def step0(m, carry):
        for w in range(2):
            if w == 1:
                ls_copy(m).wait_recv()
                ro_copy(m).wait_recv()
            for r in range(2):
                product(m, w, r, ((0, 0), (0, 1)))
        return carry

    lax.fori_loop(0, NC, step0, 0)

    def step1(m, carry):
        arrive(0, m)
        for w in range(2):
            if w == 1:
                rf_copy(0, m).wait_recv()
            for r in range(2):
                product(m, w, r, ((1, 0),))
            product(m, w, 2, ((0, 0), (0, 1), (1, 0)))
        return carry

    lax.fori_loop(0, NC, step1, 0)
    for qi in range(4):
        rs_copy(0, qi, 0).start()
    own_rows()

    def first_half(m):
        arrive(1, m)
        for w in range(2):
            for r in range(3):
                product(m, w, r, ((1, 1),))

    def second_half(m):
        for w in range(2):
            if w == 1:
                rf_copy(1, m).wait_recv()
            product(m, w, 3, ((0, 0), (0, 1), (1, 0), (1, 1)))

    first_half(0)
    second_half(0)
    reduce_step(0, 0)
    first_half(1)
    second_half(1)
    reduce_step(0, 1)
    first_half(2)
    reduce_step(0, 2)
    second_half(2)
    reduce_step(0, 3)
    finish(0, 0)
    first_half(3)
    for qi in (1, 2):
        rs_copy(1, qi, 0).start()
    second_half(3)
    for qi in (0, 3):
        rs_copy(1, qi, 0).start()
    finish(0, 1)
    gather_step(0, 2)
    gather_step(0, 1)
    reduce_step(1, 0)
    gather_step(0, 0)
    reduce_step(1, 1)
    reduce_step(1, 2)
    reduce_step(1, 3)
    finish(1, 0)
    finish(1, 1)

    lane = iota((8, 128), 1)
    pvs[0] = jnp.where(lane == 0, sums[0], jnp.where(lane == 1, sums[1], F32(0)))
    rounds = (
        (c, ((sib, 1 - c),)),
        (y, ((dims[0], y_a), (dims[2], 3 - y), (far[0], y_c))),
        (z, ((dims[1], z_a), (dims[3], 3 - z), (far[1], z_c))),
        (x, ((to_l, x_l), (to_r, x_r), (far[2], x_c))),
    )

    def pv_copy(n, i, slot):
        return pltpu.make_async_remote_copy(
            src_ref=pvs.at[n], dst_ref=pvr.at[n, slot], send_sem=pv_ss.at[n, i], recv_sem=pv_rs.at[n, slot],
            device_id=rounds[n][1][i][0], device_id_type=MESH)

    def pv_send(n):
        me, others = rounds[n]
        for i in range(len(others)):
            pv_copy(n, i, me).start()
        pvr[n, me] = pvs[n]

    def pv_sum(n):
        me, others = rounds[n]
        for i, (who, slot) in enumerate(others):
            pv_copy(n, i, slot).wait_recv()
        pvs[n + 1] = (pvr[n, 0] + pvr[n, 1]) + (pvr[n, 2] + pvr[n, 3])

    def o_copy(k, core):
        return [pltpu.make_async_copy(
            psi_v.at[pl.ds((k // 4) * 48 + (2 * l + core) * 12, 12), :, pl.ds((k % 4) * 384, 384)],
            out_hbm.at[k, pl.ds((2 * l + core) * 12, 12)], out_sem.at[k, core, l]) for l in range(2)]

    pv_send(0)
    for n, s in enumerate((2, 1, 0)):
        gather_step(1, s)
        pv_sum(n)
        pv_send(n + 1)
    for k in range(8):
        for cp in o_copy(k, c):
            cp.start()
    for g in range(2):
        for s in (3, 2, 1, 0):
            for qi in range(4):
                fw_copy(g, qi, s, 1 - c).wait_recv()
    for k in range(8):
        for cp in o_copy(k, 1 - c):
            cp.start()
    pv_sum(3)
    proj_out[...] = pvs[4]
    for g in range(2):
        for qi in range(4):
            for s in range(3):
                rs_copy(g, qi, s).wait_send()
                ag_copy(g, qi, s, True).wait_send()
            for s in range(4):
                fw_copy(g, qi, s, c).wait_send()
            if CELLS[g][qi][0] == 1:
                x_copy(g, qi).wait_send()
    for m in range(NC):
        ls_copy(m).wait_send()
        ro_copy(m).wait_send()
        for p in range(2):
            rf_copy(p, m).wait_send()
    for n in range(4):
        for i in range(len(rounds[n][1])):
            pv_copy(n, i, rounds[n][0]).wait_send()
    for k in range(8):
        for core in (c, 1 - c):
            for cp in o_copy(k, core):
                cp.wait()


def compact_body(rstart, rsize, src, out):
    x = lax.axis_index("site")
    k = pl.program_id(0)
    x_l = x + 1 - 2 * (x % 2)

    @pl.when(k == 0)
    def _():
        out[...] = jnp.zeros_like(out)

    xt = jnp.where(k // 4 == 0, x, x_l)
    site = xt + ((k // 2) % 2) * (3 - 2 * xt)
    q = site * 4 + 2 * (k % 2)
    start = rstart[q]
    base = pl.multiple_of(jnp.minimum((start // 128) * 128, BOND - 512), 128)
    j = iota((384, 512), 0)
    odd = j >= W
    idx = jnp.where(odd, j - W, j)
    size = jnp.where(odd, rsize[q + 1], rsize[q])
    first = jnp.where(odd, rstart[q + 1], start) - base
    hot = one_hot((idx < size) & (iota((384, 512), 1) == idx + first))
    out[:, pl.ds(base, 512)] += jnp.dot(src[0], hot, preferred_element_type=F32).astype(BF)


def sector_tables(sector_ids, sectors):
    labels = jnp.arange(sectors, dtype=jnp.int32)
    starts = jnp.sum((sector_ids[None, :] < labels[:, None]).astype(jnp.int32), axis=1)
    sizes = jnp.sum((sector_ids[None, :] == labels[:, None]).astype(jnp.int32), axis=1)
    return starts, sizes


def local(wavefunction, left_blocks, right_blocks, left_sector, right_sector, term_count,
          left_energy, right_energy, subspace):
    lstart, lsize = sector_tables(left_sector, 16)
    rstart, rsize = sector_tables(right_sector, 16)
    smem = pl.BlockSpec(memory_space=pltpu.SMEM)
    vmem = pl.BlockSpec(memory_space=pltpu.VMEM)
    hbm = pl.BlockSpec(memory_space=pl.ANY)
    dma = pltpu.SemaphoreType.DMA
    slabs, proj = pl.pallas_call(
        body,
        out_shape=(jax.ShapeDtypeStruct((8, 48, 16, 384), BF), jax.ShapeDtypeStruct((8, 128), F32)),
        in_specs=[smem] * 5 + [hbm] * 3 + [vmem] * 2 + [hbm],
        out_specs=(hbm, vmem),
        scratch_shapes=[
            pltpu.VMEM((BOND // 16, 16, BOND), BF),
            pltpu.VMEM((16, 1024, 128), BF),
            pltpu.VMEM((8, 1024, 256), BF),
            pltpu.VMEM((2, 2, NS, 4, W, W), BF),
            pltpu.VMEM((5, SLOTS, 3, W, 128), BF),
            pltpu.VMEM((4, 2, SLOTS, 3, 320, 128), BF),
            pltpu.VMEM((768, NS * 256), BF),
            pltpu.VMEM((2, 4, 384, 384), F32),
            pltpu.VMEM((8, 2, 48, BOND), BF),
            pltpu.VMEM((8, 48, 384), F32),
            pltpu.VMEM((8, 2, 48, 384), F32),
            pltpu.VMEM((2, 4, 192, 384), F32),
            pltpu.VMEM((2, 4, 96, 384), F32),
            pltpu.VMEM((2, 4, 48, 384), F32),
            pltpu.VMEM((2, 4, 48, 384), F32),
            pltpu.VMEM((2, 4, 48, 384), F32),
            pltpu.VMEM((5, 8, 128), F32),
            pltpu.VMEM((4, 4, 8, 128), F32),
            dma((2, 2)), dma, dma((8, 2)), dma((8, 2, 2)),
            dma((2, NC, 2)), dma((2, NC, 2)), dma((NC,)), dma((NC,)), dma((2, NC)), dma((2, NC)),
            dma((NC,)), dma((NC,)), dma((2, NC)), dma((2, NC)),
            dma((2, 4, 4)), dma((2, 4, 4)), dma((2, 4)), dma((2, 4)),
            dma((2, 4, 3)), dma((2, 4, 3)), dma((2, 4, 4)), dma((2, 4, 4)), dma((4, 3)), dma((4, 4)),
        ],
        compiler_params=pltpu.CompilerParams(
            collective_id=0, has_side_effects=True, vmem_limit_bytes=67043328),
        name="exchange",
    )(lstart, lsize, rstart, rsize, term_count, wavefunction.reshape(BOND // 16, 16, BOND),
      left_blocks, right_blocks, left_energy.reshape(16, 1, 128), right_energy.reshape(1, BOND), subspace)
    sigma = pl.pallas_call(
        compact_body,
        grid=(8,),
        out_shape=jax.ShapeDtypeStruct((768, BOND), BF),
        in_specs=[smem, smem, pl.BlockSpec((1, 768, 384), lambda k: (k, 0, 0))],
        out_specs=pl.BlockSpec((768, BOND), lambda k: (0, 0)),
        name="compact",
    )(rstart, rsize, slabs.reshape(8, 768, 384))
    return sigma.reshape(4, W, BOND), proj[0, :2]


def solution(mesh):
    in_specs = (P(), P("ops", "site", None, None), P("ops", "site", None, None), P(), P(), P("ops"),
                P(), P(), P(None, "site", None, None))
    out_specs = (P("site", None, None), P())
    return jax.shard_map(local, mesh=mesh, in_specs=in_specs, out_specs=out_specs, check_vma=False)
```

```python
import jax
import jax.numpy as jnp
from jax import lax
from jax.experimental import pallas as pl
from jax.experimental.pallas import tpu as pltpu
from jax.sharding import PartitionSpec as P

W = 192
SLOTS = 8
NS = 2
NC = SLOTS // NS
BOND = 2048
BF = jnp.bfloat16
F32 = jnp.float32
MESH = pl.DeviceIdType.MESH


def iota(shape, dim):
    return lax.broadcasted_iota(jnp.int32, shape, dim)


def one_hot(mask):
    return jnp.where(mask, F32(1), F32(0)).astype(BF)


def packed_index(pos, parity):
    tail = pos - 64 * parity
    idx = jnp.where(pos < 128, pos, tail)
    ok = (pos < 128) | ((tail >= 128) & (tail < W))
    return idx, ok


CELLS = (
    ((0, ((0, 0),)), (0, ((0, 1),)), (0, ((1, 0),)), (0, ((1, 1),))),
    ((0, ((0, 2),)), (0, ((1, 2),)), (1, ((0, 0),)), (1, ((0, 1),))),
    ((0, ((0, 3), (1, 3))), (1, ((1, 0), (1, 1))), (1, ((0, 2), (1, 2))), (1, ((0, 3), (1, 3)))),
)
CHUNKS = len(CELLS)
BASE = (0, 4, 8)
PLACE = {
    (h, l, r): BASE[g] + q * len(cells) + n
    for g in range(CHUNKS) for q, (h, cells) in enumerate(CELLS[g]) for n, (l, r) in enumerate(cells)
}
STEPS = ((96, 48), (96, 48), (192, 96, 48))
PARTS = (((0, 384),), ((0, 384),), ((0, 256), (256, 128)))


def piece_offsets(bits):
    offs = []
    for g in range(CHUNKS):
        offs.append([])
        for qi in range(4):
            off = [0]
            for s, rows in enumerate(STEPS[g]):
                off.append(off[-1] + bits[(qi + s) % 4] * rows)
            offs[g].append(off)
    return offs


def cell_at(g, qi, n):
    cells = CELLS[g][qi][1]
    (l0, r0), (l1, r1) = cells[0], cells[-1]
    return l0 + n * (l1 - l0), r0 + n * (r1 - r0)


def label_bits(y, z):
    return (((y + 1) // 2) % 2, ((z + 1) // 2) % 2, y // 2, z // 2)


def body(
    lstart, lsize, rstart, rsize, count,
    psi_hbm, left_hbm, right_hbm, lenergy, renergy, sub_hbm,
    out_hbm, proj_out,
    psi_v, gath, pp, raw, lall, rb, li, acc, subv, diag, subp,
    rs0, rs1, rs2, rs3, rs4, xrecv, pvs, pvr,
    raw_sem, psi_sem, sub_sem, out_sem,
    l_ss, l_rs, ls_ss, ls_rs, r_ss, r_rs, ro_ss, ro_rs, rf_ss, rf_rs, rs_ss, rs_rs, x_ss, x_rs,
    ag_ss, ag_rs, fw_ss, fw_rs, pv_ss, pv_rs,
):
    x = lax.axis_index("site")
    o = lax.axis_index("ops")
    c = o % 2
    y = (o // 2) % 4
    z = o // 8
    x_l = x + 1 - 2 * (x % 2)
    x_r = 3 - x
    to_l = {"site": x_l}
    to_r = {"site": x_r}
    sib = {"ops": o + 1 - 2 * c}
    to_ls = {"ops": o + 1 - 2 * c, "site": x_l}
    y_a = y + 1 - 2 * (y % 2)
    z_a = z + 1 - 2 * (z % 2)
    y_c = 3 - y_a
    z_c = 3 - z_a
    x_c = 3 - x_l
    dims = (
        {"ops": o + 2 * (y_a - y)},
        {"ops": o + 8 * (z_a - z)},
        {"ops": o + 2 * (3 - 2 * y)},
        {"ops": o + 8 * (3 - 2 * z)},
    )
    far = ({"ops": o + 2 * (y_c - y)}, {"ops": o + 8 * (z_c - z)}, {"site": x_c})
    bits = label_bits(y, z)
    offs = piece_offsets(bits)
    data = pl.ds(64, W)

    def raw_copies(m):
        buf = m % 2
        return (
            pltpu.make_async_copy(left_hbm.at[pl.ds(NS * m, NS)], raw.at[buf, 0], raw_sem.at[buf, 0]),
            pltpu.make_async_copy(right_hbm.at[pl.ds(NS * m, NS)], raw.at[buf, 1], raw_sem.at[buf, 1]),
        )

    for m in range(2):
        for cp in raw_copies(m):
            cp.start()
    psi_copy = pltpu.make_async_copy(psi_hbm, psi_v, psi_sem)
    psi_copy.start()

    pvr[...] = jnp.zeros_like(pvr)
    barrier = pltpu.get_barrier_semaphore()
    for who in (to_l, to_r, sib, to_ls, *dims, *far):
        pl.semaphore_signal(barrier, inc=1, device_id=who, device_id_type=MESH)

    def l_copy(ph, m, w):
        at = pl.ds(NS * m, NS)
        tiles = pl.ds(0, 2) if ph == 0 else pl.ds(2, 1)
        return pltpu.make_async_remote_copy(
            src_ref=lall.at[c if w == 0 else 1 - c, at, tiles], dst_ref=lall.at[3 + w, at, tiles],
            send_sem=l_ss.at[ph, m, w], recv_sem=l_rs.at[ph, m, w],
            device_id=to_l if w == 0 else to_ls, device_id_type=MESH)

    def ls_copy(m):
        at = pl.ds(NS * m, NS)
        return pltpu.make_async_remote_copy(
            src_ref=lall.at[1 - c, at], dst_ref=lall.at[2, at], send_sem=ls_ss.at[m], recv_sem=ls_rs.at[m],
            device_id=sib, device_id_type=MESH)

    def r_copy(p, m):
        at = pl.ds(NS * m, NS)
        return pltpu.make_async_remote_copy(
            src_ref=rb.at[0, p, at, :, data, :], dst_ref=rb.at[2, p, at, :, data, :],
            send_sem=r_ss.at[p, m], recv_sem=r_rs.at[p, m], device_id=to_r, device_id_type=MESH)

    def ro_copy(m):
        at = pl.ds(NS * m, NS)
        return pltpu.make_async_remote_copy(
            src_ref=rb.at[0, :, at, :, data, :], dst_ref=rb.at[1, :, at, :, data, :],
            send_sem=ro_ss.at[m], recv_sem=ro_rs.at[m], device_id=sib, device_id_type=MESH)

    def rf_copy(p, m):
        at = pl.ds(NS * m, NS)
        return pltpu.make_async_remote_copy(
            src_ref=rb.at[2, p, at, :, data, :], dst_ref=rb.at[3, p, at, :, data, :],
            send_sem=rf_ss.at[p, m], recv_sem=rf_rs.at[p, m], device_id=sib, device_id_type=MESH)

    def pack(m):
        buf = m % 2

        def one(k, carry):
            s = k // 2
            p = k % 2
            slot = NS * m + s
            row = iota((W, 128), 0)
            live = slot < count[0]
            keep = []
            for n in range(2):
                size = jnp.where(live, lsize[x * 4 + 2 * n + p], 0)
                keep.append(one_hot(row < size))
            ev = raw[buf, 0, s, p]
            od = raw[buf, 0, s, 2 + p]
            lall[p, slot, 0] = ev[:, :128] * keep[0]
            lall[p, slot, 2] = od[:, :128] * keep[1]
            lall[p, slot, 1] = jnp.concatenate(
                [ev[:, 128:] * keep[0][:, :64], od[:, 128:] * keep[1][:, :64]], axis=1)
            ev = raw[buf, 1, s, 2 * p]
            od = raw[buf, 1, s, 2 * p + 1]
            rb[0, p, slot, 0, data, :] = ev[:, :128]
            rb[0, p, slot, 1, data, :] = od[:, :128]
            rb[0, p, slot, 2, data, :] = jnp.concatenate([ev[:, 128:], od[:, 128:]], axis=1)
            return carry

        lax.fori_loop(0, 2 * NS, one, 0)

    for m in range(NC):
        for cp in raw_copies(m):
            cp.wait()
        pack(m)
        if m == 0:
            pl.semaphore_wait(barrier, 11)
        if m + 2 < NC:
            for cp in raw_copies(m + 2):
                cp.start()
        for w in range(2):
            l_copy(0, m, w).start()
        r_copy(0, m).start()
        ls_copy(m).start()
        ro_copy(m).start()
    for m in range(NC):
        for w in range(2):
            l_copy(1, m, w).start()
        r_copy(1, m).start()

    def piece(g, qi):
        off = offs[g][qi][-1]
        n = off // W
        l, r = cell_at(g, qi, n)
        return 2 * l + c, off - n * W, r

    def sub_copy(g, qi, k):
        i, a0, r = piece(g, qi)
        return pltpu.make_async_copy(
            sub_hbm.at[k, i, pl.ds(pl.multiple_of(a0, 16), 48), :],
            subv.at[g * 4 + qi, k], sub_sem.at[g * 4 + qi, k])

    for g in range(CHUNKS):
        for qi in range(4):
            for k in range(2):
                sub_copy(g, qi, k).start()

    zrow = jnp.zeros((SLOTS, 3, 64, 128), BF)

    def clear(k, carry):
        for start in (0, 256):
            rb[k // 2, k % 2, :, :, pl.ds(start, 64), :] = zrow
        acc[2 * k] = jnp.zeros((W, 384), F32)
        acc[2 * k + 1] = jnp.zeros((W, 384), F32)
        return carry

    lax.fori_loop(0, 8, clear, 0)

    psi_copy.wait()

    def row_hot(q, first, rows, half):
        rs = lstart[q]
        t0 = jnp.minimum(rs // 16, BOND // 16 - 16)
        pos = iota((rows, 256), 0) + first
        if half is None:
            idx, ok = pos, pos < W
        else:
            idx, ok = packed_index(pos, half)
        ok = ok & (idx < lsize[q])
        return t0, one_hot(ok & (iota((rows, 256), 1) == idx + (rs - t0 * 16)))

    def put_rows(at, rows, t0, hot):
        for n in range(4):
            win = jnp.concatenate([psi_v[t0 + k, :, pl.ds(n * 512, 512)] for k in range(16)], axis=0)
            got = jnp.dot(hot, win, preferred_element_type=F32).astype(BF)
            for k in range(4):
                gath[n * 4 + k, pl.ds(at, rows), :] = got[:, k * 128:(k + 1) * 128]

    def rows_of(i, carry):
        q = jnp.where(i < 2, x, x_l) * 4 + 2 * (i % 2) + c
        t0, hot = row_hot(q, 0, 256, i % 2)
        put_rows(pl.multiple_of(i * 256, 256), 256, t0, hot)
        return carry

    lax.fori_loop(0, 4, rows_of, 0)

    def cols_of(j, carry):
        q = jnp.where(j < 4, x * 4 + j, x_r * 4 + j - 4)
        cs = rstart[q]
        ct = jnp.minimum(cs // 128, BOND // 128 - 3)
        idx, ok = packed_index(iota((384, 256), 1), q % 2)
        ok = ok & (idx < rsize[q])
        hot = one_hot(ok & (iota((384, 256), 0) == idx + (cs - ct * 128)))
        for m in range(2):
            win = jnp.concatenate([gath[ct + k, pl.ds(m * 512, 512), :] for k in range(3)], axis=1)
            pp[j, pl.ds(m * 512, 512), :] = jnp.dot(win, hot, preferred_element_type=F32).astype(BF)
        return carry

    lax.fori_loop(0, 8, cols_of, 0)

    def own_rows():
        re = renergy[...]
        hi = re.astype(BF)
        rem = re - hi.astype(F32)
        mid = rem.astype(BF)
        low = (rem - mid.astype(F32)).astype(BF)
        rows16 = iota((16, BOND), 0)
        er3 = jnp.where(rows16 == 0, hi.astype(F32),
                        jnp.where(rows16 == 1, mid.astype(F32),
                                  jnp.where(rows16 == 2, low.astype(F32), F32(0)))).astype(BF)
        for t in range(16):
            for qi in range(4):
                gath[t, pl.ds(qi * 160 + 144, 16), :] = er3[:, t * 128:(t + 1) * 128]
        for g in range(CHUNKS):
            for qi in range(4):
                n8 = g * 4 + qi
                at = qi * 160
                i, a0, r = piece(g, qi)
                q = x * 4 + i
                t0, hot = row_hot(q, a0, 48, None)
                put_rows(at, 48, t0, hot)
                for k in range(2):
                    sub_copy(g, qi, k).wait()
                    for t in range(16):
                        gath[t, pl.ds(at + 48 + 48 * k, 48), :] = subv[n8, k, :, pl.ds(t * 128, 128)]
                xt = x if CELLS[g][qi][0] == 0 else x_l
                site = xt + (r // 2) * (3 - 2 * xt)
                total = None
                for par in range(2):
                    qr = site * 4 + 2 * (r % 2) + par
                    cs = rstart[qr]
                    ct = jnp.minimum(cs // 128, BOND // 128 - 3)
                    j = iota((384, 384), 1) - W * par
                    hot2 = one_hot((j >= 0) & (j < W) & (j < rsize[qr])
                                   & (iota((384, 384), 0) == j + (cs - ct * 128)))
                    win = jnp.concatenate([gath[ct + k, pl.ds(at, 160), :] for k in range(3)], axis=1)
                    part = jnp.dot(win, hot2, preferred_element_type=F32)
                    total = part if total is None else total + part
                lt = jnp.minimum(lstart[q] // 128, BOND // 128 - 3)
                shift = lstart[q] - lt * 128 + a0
                pick = iota((48, 384), 1) == iota((48, 384), 0) + shift
                lrow = jnp.concatenate([lenergy[lt + k] for k in range(3)], axis=1)
                el = jnp.sum(jnp.where(pick, lrow, F32(0)), axis=1, keepdims=True)
                er = total[144:145] + total[145:146] + total[146:147]
                diag[n8] = (el + er) * total[:48]
                subp[n8, 0] = total[48:96]
                subp[n8, 1] = total[96:144]

    left_at = {(0, 0): c, (0, 1): 2, (1, 0): 3, (1, 1): 4}

    def product(m, w, r, lefts):
        slots = pl.ds(NS * m, NS)
        side = (0 if r < 2 else 2) + w
        for par in range(2):
            j = 2 * r + par
            for n, (h, l) in enumerate(lefts):
                src = left_at[(h, w)]
                lhs = jnp.concatenate([lall[src, slots, 2 * l].reshape(NS * W, 128),
                                       lall[src, slots, 1].reshape(NS * W, 128)], axis=1)
                img = jnp.dot(lhs, pp[j, pl.ds((2 * h + l) * 256, 256), :],
                              preferred_element_type=F32).astype(BF)
                for s in range(NS):
                    li[pl.ds(n * W, W), pl.ds(s * 256, 256)] = img[s * W:(s + 1) * W]
            rows = pl.ds(64 - 64 * par, 256)
            rhs = jnp.concatenate(
                [rb[side, r % 2, NS * m + s, k, rows, :] for s in range(NS) for k in (par, 2)], axis=1)
            lanes = pl.ds(128 * par, 256)
            res = lax.dot_general(li[pl.ds(0, len(lefts) * W), :], rhs, (((1,), (1,)), ((), ())),
                                  preferred_element_type=F32)
            for n, (h, l) in enumerate(lefts):
                acc[PLACE[(h, l, r)], :, lanes] += res[n * W:(n + 1) * W]

    def arrive(p, m):
        r_copy(p, m).wait()
        rf_copy(p, m).start()
        for w in range(2):
            l_copy(p, m, w).wait()

    def landing(g, qi, s):
        steps = STEPS[g]
        if s == 3:
            return rs3.at[g, qi], 48, True
        if s == len(steps):
            return rs4.at[g, qi], 48, True
        rows = steps[s]
        return {192: rs0.at[qi], 96: rs1.at[g, qi], 48: rs2.at[g, qi]}[rows], rows, False

    def lanes_of(g, pt, first=0):
        start, width = PARTS[g][pt]
        return pl.ds(pl.multiple_of(first + start, 128), width)

    def strip(g, qi, first, rows):
        n = first // W
        return BASE[g] + qi * len(CELLS[g][qi][1]) + n, pl.ds(pl.multiple_of(first - n * W, 16), rows)

    def rs_copy(g, qi, s, pt):
        d = (qi + s) % 4
        dst, rows, whole = landing(g, qi, s)
        first = offs[g][qi][-1] if whole else offs[g][qi][s] + (1 - bits[d]) * rows
        n, at = strip(g, qi, first, rows)
        return pltpu.make_async_remote_copy(
            src_ref=acc.at[n, at, lanes_of(g, pt)], dst_ref=dst.at[:, lanes_of(g, pt)],
            send_sem=rs_ss.at[g, qi, s, pt], recv_sem=rs_rs.at[g, qi, s, pt],
            device_id=dims[d], device_id_type=MESH)

    def add_rows(g, qi, first, src, rows, pt):
        lanes = lanes_of(g, pt)
        n = first // W
        row = first - n * W
        n = BASE[g] + qi * len(CELLS[g][qi][1]) + n

        def step(k, carry):
            at = pl.ds(pl.multiple_of(row + k * 48, 16), 48)
            acc[n, at, lanes] += src[pl.ds(pl.multiple_of(k * 48, 16), 48), lanes]
            return carry

        lax.fori_loop(0, rows // 48, step, 0)

    def x_copy(g, qi, pt):
        lanes = lanes_of(g, pt)
        n, at = strip(g, qi, offs[g][qi][-1], 48)
        return pltpu.make_async_remote_copy(
            src_ref=acc.at[n, at, lanes], dst_ref=xrecv.at[g, qi, :, lanes],
            send_sem=x_ss.at[g, qi, pt], recv_sem=x_rs.at[g, qi, pt], device_id=to_l, device_id_type=MESH)

    def reduce_step(g, s, pt=0):
        for qi in range(4):
            src, rows, whole = landing(g, qi, s)
            rs_copy(g, qi, s, pt).wait_recv()
            if whole:
                rs_copy(g, qi, s, pt).wait_send()
            add_rows(g, qi, offs[g][qi][-1] if whole else offs[g][qi][s + 1], src, rows, pt)
            if s < 3:
                rs_copy(g, qi, s + 1, pt).start()
            elif CELLS[g][qi][0] == 1:
                x_copy(g, qi, pt).start()

    def rows_at(g, qi, first, rows, core, pt):
        n = first // W
        l, r = cell_at(g, qi, n)
        tile = CELLS[g][qi][0] * 48 + (2 * l + core) * 12 + (first - n * W) // 16
        return pl.ds(tile, rows // 16), lanes_of(g, pt, r * 384)

    def ag_copy(g, qi, s, mine, pt):
        d = (qi + s) % 4
        rows = STEPS[g][s]
        first = offs[g][qi][s + 1] if mine else offs[g][qi][s] + (1 - bits[d]) * rows
        at, lanes = rows_at(g, qi, first, rows, c, pt)
        return pltpu.make_async_remote_copy(
            src_ref=psi_v.at[at, :, lanes], dst_ref=psi_v.at[at, :, lanes],
            send_sem=ag_ss.at[g, qi, s, pt], recv_sem=ag_rs.at[g, qi, s, pt],
            device_id=dims[d], device_id_type=MESH)

    def fw_copy(g, qi, s, core, pt):
        if s == 3:
            first, rows = offs[g][qi][-1], 48
        else:
            rows = STEPS[g][s]
            first = offs[g][qi][s] + (1 - bits[(qi + s) % 4]) * rows
        at, lanes = rows_at(g, qi, first, rows, core, pt)
        return pltpu.make_async_remote_copy(
            src_ref=psi_v.at[at, :, lanes], dst_ref=psi_v.at[at, :, lanes],
            send_sem=fw_ss.at[g, qi, s, pt], recv_sem=fw_rs.at[g, qi, s, pt],
            device_id=sib, device_id_type=MESH)

    totals = [jnp.zeros((48, 128), F32), jnp.zeros((48, 128), F32)]

    def finish(g, h, pt=0):
        lanes = lanes_of(g, pt)
        for qi in range(4):
            if CELLS[g][qi][0] != h:
                continue
            off = offs[g][qi][-1]
            if h == 0:
                n, rows = strip(g, qi, off, 48)
                part = acc[n, rows, lanes]
            else:
                x_copy(g, qi, pt).wait_recv()
                part = xrecv[g, qi, :, lanes]
            full = part + diag[g * 4 + qi, :, lanes]
            at, where = rows_at(g, qi, off, 48, c, pt)
            width = PARTS[g][pt][1]
            psi_v[at, :, where] = full.astype(BF).reshape(3, 16, width)
            ag_copy(g, qi, len(STEPS[g]) - 1, True, pt).start()
            fw_copy(g, qi, 3, c, pt).start()
            weight = 1 - bits[(qi + 3) % 4]
            if len(STEPS[g]) == 2:
                weight = weight * (1 - bits[(qi + 2) % 4])
            weight = weight.astype(F32)
            for k in range(2):
                prod = weight * full * subp[g * 4 + qi, k, :, lanes]
                for t in range(width // 128):
                    totals[k] = totals[k] + prod[:, t * 128:(t + 1) * 128]

    def gather_step(g, s, pt=0):
        for qi in range(4):
            ag_copy(g, qi, s, False, pt).wait_recv()
            if s > 0:
                ag_copy(g, qi, s - 1, True, pt).start()
            fw_copy(g, qi, s, c, pt).start()

    def step0(m, carry):
        for w in range(2):
            if w == 1:
                ls_copy(m).wait_recv()
                ro_copy(m).wait_recv()
            for r in range(2):
                product(m, w, r, ((0, 0), (0, 1)))
        return carry

    lax.fori_loop(0, NC, step0, 0)
    for qi in range(4):
        rs_copy(0, qi, 0, 0).start()
    own_rows()
    reduce_step(0, 0)

    def step1(m, carry):
        arrive(0, m)
        for w in range(2):
            if w == 1:
                rf_copy(0, m).wait_recv()
            for r in range(2):
                product(m, w, r, ((1, 0),))
            product(m, w, 2, ((0, 0), (0, 1), (1, 0)))
        return carry

    lax.fori_loop(0, NC // 2, step1, 0)
    reduce_step(0, 1)
    lax.fori_loop(NC // 2, NC, step1, 0)
    for qi in range(4):
        rs_copy(1, qi, 0, 0).start()
    reduce_step(0, 2)

    def first_half(m):
        arrive(1, m)
        for w in range(2):
            for r in range(3):
                product(m, w, r, ((1, 1),))

    def second_half(m):
        for w in range(2):
            if w == 1:
                rf_copy(1, m).wait_recv()
            product(m, w, 3, ((0, 0), (0, 1), (1, 0), (1, 1)))

    first_half(0)
    reduce_step(0, 3)
    finish(0, 0)
    second_half(0)
    reduce_step(1, 0)
    gather_step(0, 1)
    first_half(1)
    second_half(1)
    reduce_step(1, 1)
    gather_step(0, 0)
    first_half(2)
    second_half(2)
    reduce_step(1, 2)
    first_half(3)
    for qi in (1, 2):
        for pt in range(2):
            rs_copy(2, qi, 0, pt).start()
    second_half(3)
    for qi in (0, 3):
        for pt in range(2):
            rs_copy(2, qi, 0, pt).start()
    reduce_step(1, 3)
    finish(1, 0)
    reduce_step(2, 0, 0)
    finish(1, 1)
    reduce_step(2, 0, 1)
    reduce_step(2, 1, 0)
    gather_step(1, 1)
    reduce_step(2, 1, 1)
    reduce_step(2, 2, 0)
    gather_step(1, 0)
    reduce_step(2, 2, 1)
    for pt in range(2):
        reduce_step(2, 3, pt)
    for pt in range(2):
        finish(2, 0, pt)
        finish(2, 1, pt)

    lane = iota((8, 128), 1)
    sums = [jnp.sum(total, keepdims=True) for total in totals]
    pvs[0] = jnp.where(lane == 0, sums[0], jnp.where(lane == 1, sums[1], F32(0)))
    rounds = (
        (c, ((sib, 1 - c),)),
        (y, ((dims[0], y_a), (dims[2], 3 - y), (far[0], y_c))),
        (z, ((dims[1], z_a), (dims[3], 3 - z), (far[1], z_c))),
        (x, ((to_l, x_l), (to_r, x_r), (far[2], x_c))),
    )

    def pv_copy(n, i, slot):
        return pltpu.make_async_remote_copy(
            src_ref=pvs.at[n], dst_ref=pvr.at[n, slot], send_sem=pv_ss.at[n, i], recv_sem=pv_rs.at[n, slot],
            device_id=rounds[n][1][i][0], device_id_type=MESH)

    def pv_send(n):
        me, others = rounds[n]
        for i in range(len(others)):
            pv_copy(n, i, me).start()
        pvr[n, me] = pvs[n]

    def pv_sum(n):
        me, others = rounds[n]
        for i, (who, slot) in enumerate(others):
            pv_copy(n, i, slot).wait_recv()
        pvs[n + 1] = (pvr[n, 0] + pvr[n, 1]) + (pvr[n, 2] + pvr[n, 3])

    def o_copy(k, core):
        return [pltpu.make_async_copy(
            psi_v.at[pl.ds((k // 4) * 48 + (2 * l + core) * 12, 12), :, pl.ds((k % 4) * 384, 384)],
            out_hbm.at[k, pl.ds((2 * l + core) * 12, 12)], out_sem.at[k, core, l]) for l in range(2)]

    pv_send(0)
    for n, s in enumerate((2, 1, 0)):
        for pt in range(2):
            gather_step(2, s, pt)
        pv_sum(n)
        pv_send(n + 1)
    for k in range(8):
        for cp in o_copy(k, c):
            cp.start()
    for g in range(CHUNKS):
        for s in (3, *reversed(range(len(STEPS[g])))):
            for qi in range(4):
                for pt in range(len(PARTS[g])):
                    fw_copy(g, qi, s, 1 - c, pt).wait_recv()
    for k in range(8):
        for cp in o_copy(k, 1 - c):
            cp.start()
    pv_sum(3)
    proj_out[...] = pvs[4]
    for g in range(CHUNKS):
        for qi in range(4):
            for pt in range(len(PARTS[g])):
                for s in range(len(STEPS[g])):
                    rs_copy(g, qi, s, pt).wait_send()
                    ag_copy(g, qi, s, True, pt).wait_send()
                    fw_copy(g, qi, s, c, pt).wait_send()
                fw_copy(g, qi, 3, c, pt).wait_send()
                if CELLS[g][qi][0] == 1:
                    x_copy(g, qi, pt).wait_send()
    for m in range(NC):
        ls_copy(m).wait_send()
        ro_copy(m).wait_send()
        for p in range(2):
            rf_copy(p, m).wait_send()
    for n in range(4):
        for i in range(len(rounds[n][1])):
            pv_copy(n, i, rounds[n][0]).wait_send()
    for k in range(8):
        for core in (c, 1 - c):
            for cp in o_copy(k, core):
                cp.wait()


def compact_body(rstart, rsize, proj, src, out, proj_out):
    x = lax.axis_index("site")
    k = pl.program_id(0)
    x_l = x + 1 - 2 * (x % 2)

    @pl.when(k == 0)
    def _():
        out[...] = jnp.zeros_like(out)
        for i in range(2):
            proj_out[i] = proj[0, i]

    xt = jnp.where(k // 4 == 0, x, x_l)
    site = xt + ((k // 2) % 2) * (3 - 2 * xt)
    q = site * 4 + 2 * (k % 2)
    start = rstart[q]
    base = pl.multiple_of(jnp.minimum((start // 128) * 128, BOND - 512), 128)
    j = iota((384, 1), 0)
    odd = j >= W
    idx = jnp.where(odd, j - W, j)
    size = jnp.where(odd, rsize[q + 1], rsize[q])
    first = jnp.where(odd, rstart[q + 1], start) - base
    target = jnp.where(idx < size, idx + first, -1)
    hot = one_hot(iota((384, 512), 1) == target)
    out[:, pl.ds(base, 512)] += jnp.dot(src[0], hot, preferred_element_type=F32).astype(BF)


def sector_tables(sector_ids, sectors):
    labels = jnp.arange(sectors, dtype=jnp.int32)
    starts = jnp.sum((sector_ids[None, :] < labels[:, None]).astype(jnp.int32), axis=1)
    sizes = jnp.sum((sector_ids[None, :] == labels[:, None]).astype(jnp.int32), axis=1)
    return starts, sizes


def local(wavefunction, left_blocks, right_blocks, left_sector, right_sector, term_count,
          left_energy, right_energy, subspace):
    lstart, lsize = sector_tables(left_sector, 16)
    rstart, rsize = sector_tables(right_sector, 16)
    smem = pl.BlockSpec(memory_space=pltpu.SMEM)
    vmem = pl.BlockSpec(memory_space=pltpu.VMEM)
    hbm = pl.BlockSpec(memory_space=pl.ANY)
    dma = pltpu.SemaphoreType.DMA
    slabs, proj = pl.pallas_call(
        body,
        out_shape=(jax.ShapeDtypeStruct((8, 48, 16, 384), BF), jax.ShapeDtypeStruct((8, 128), F32)),
        in_specs=[smem] * 5 + [hbm] * 3 + [vmem] * 2 + [hbm],
        out_specs=(hbm, vmem),
        scratch_shapes=[
            pltpu.VMEM((BOND // 16, 16, BOND), BF),
            pltpu.VMEM((16, 1024, 128), BF),
            pltpu.VMEM((8, 1024, 256), BF),
            pltpu.VMEM((2, 2, NS, 4, W, W), BF),
            pltpu.VMEM((5, SLOTS, 3, W, 128), BF),
            pltpu.VMEM((4, 2, SLOTS, 3, 320, 128), BF),
            pltpu.VMEM((768, NS * 256), BF),
            pltpu.VMEM((16, W, 384), F32),
            pltpu.VMEM((12, 2, 48, BOND), BF),
            pltpu.VMEM((12, 48, 384), F32),
            pltpu.VMEM((12, 2, 48, 384), F32),
            pltpu.VMEM((4, 192, 384), F32),
            pltpu.VMEM((3, 4, 96, 384), F32),
            pltpu.VMEM((3, 4, 48, 384), F32),
            pltpu.VMEM((3, 4, 48, 384), F32),
            pltpu.VMEM((2, 4, 48, 384), F32),
            pltpu.VMEM((3, 4, 48, 384), F32),
            pltpu.VMEM((5, 8, 128), F32),
            pltpu.VMEM((4, 4, 8, 128), F32),
            dma((2, 2)), dma, dma((12, 2)), dma((8, 2, 2)),
            dma((2, NC, 2)), dma((2, NC, 2)), dma((NC,)), dma((NC,)), dma((2, NC)), dma((2, NC)),
            dma((NC,)), dma((NC,)), dma((2, NC)), dma((2, NC)),
            dma((3, 4, 4, 2)), dma((3, 4, 4, 2)), dma((3, 4, 2)), dma((3, 4, 2)),
            dma((3, 4, 3, 2)), dma((3, 4, 3, 2)), dma((3, 4, 4, 2)), dma((3, 4, 4, 2)), dma((4, 3)), dma((4, 4)),
        ],
        compiler_params=pltpu.CompilerParams(
            collective_id=0, has_side_effects=True, vmem_limit_bytes=67043328),
        name="exchange",
    )(lstart, lsize, rstart, rsize, term_count, wavefunction.reshape(BOND // 16, 16, BOND),
      left_blocks, right_blocks, left_energy.reshape(16, 1, 128), right_energy.reshape(1, BOND), subspace)
    sigma, projections = pl.pallas_call(
        compact_body,
        grid=(8,),
        out_shape=(jax.ShapeDtypeStruct((768, BOND), BF), jax.ShapeDtypeStruct((2,), F32)),
        in_specs=[smem, smem, smem, pl.BlockSpec((1, 768, 384), lambda k: (k, 0, 0))],
        out_specs=(pl.BlockSpec((768, BOND), lambda k: (0, 0)), smem),
        name="compact",
    )(rstart, rsize, proj, slabs.reshape(8, 768, 384))
    return sigma.reshape(4, W, BOND), projections


def solution(mesh):
    in_specs = (P(), P("ops", "site", None, None), P("ops", "site", None, None), P(), P(), P("ops"),
                P(), P(), P(None, "site", None, None))
    out_specs = (P("site", None, None), P())
    return jax.shard_map(local, mesh=mesh, in_specs=in_specs, out_specs=out_specs, check_vma=False)
```

```python
import jax
import jax.numpy as jnp
from jax import lax
from jax.experimental import pallas as pl
from jax.experimental.pallas import tpu as pltpu
from jax.sharding import PartitionSpec as P

W = 192
SLOTS = 8
NS = 2
NC = SLOTS // NS
BOND = 2048
BF = jnp.bfloat16
F32 = jnp.float32
MESH = pl.DeviceIdType.MESH


def iota(shape, dim):
    return lax.broadcasted_iota(jnp.int32, shape, dim)


def one_hot(mask):
    return jnp.where(mask, F32(1), F32(0)).astype(BF)


def packed_index(pos, parity):
    tail = pos - 64 * parity
    idx = jnp.where(pos < 128, pos, tail)
    ok = (pos < 128) | ((tail >= 128) & (tail < W))
    return idx, ok


CELLS = (
    ((0, ((0, 0),)), (0, ((0, 1),)), (0, ((1, 0),)), (0, ((1, 1),))),
    ((0, ((0, 2),)), (0, ((1, 2),)), (1, ((0, 0),)), (1, ((0, 1),))),
    ((0, ((0, 3), (1, 3))), (1, ((1, 0), (1, 1))), (1, ((0, 2), (1, 2))), (1, ((0, 3), (1, 3)))),
)
CHUNKS = len(CELLS)
BASE = (0, 4, 8)
PLACE = {
    (h, l, r): BASE[g] + q * len(cells) + n
    for g in range(CHUNKS) for q, (h, cells) in enumerate(CELLS[g]) for n, (l, r) in enumerate(cells)
}
STEPS = ((96, 48), (96, 48), (192, 96, 48))
PARTS = (((0, 384),), ((0, 384),), ((0, 256), (256, 128)))


def piece_offsets(bits):
    offs = []
    for g in range(CHUNKS):
        offs.append([])
        for qi in range(4):
            off = [0]
            for s, rows in enumerate(STEPS[g]):
                off.append(off[-1] + bits[(qi + s) % 4] * rows)
            offs[g].append(off)
    return offs


def cell_at(g, qi, n):
    cells = CELLS[g][qi][1]
    (l0, r0), (l1, r1) = cells[0], cells[-1]
    return l0 + n * (l1 - l0), r0 + n * (r1 - r0)


def label_bits(y, z):
    return (((y + 1) // 2) % 2, ((z + 1) // 2) % 2, y // 2, z // 2)


def body(
    lstart, lsize, rstart, rsize, count,
    psi_hbm, left_hbm, right_hbm, lenergy, renergy, sub_hbm,
    out_hbm, proj_out,
    psi_v, gath, pp, raw, lall, rb, li, acc, subv, diag, subp,
    rs0, rs1, rs2, rs3, rs4, xrecv, pvs, pvr,
    raw_sem, psi_sem, sub_sem, out_sem,
    l_ss, l_rs, ls_ss, ls_rs, r_ss, r_rs, ro_ss, ro_rs, rf_ss, rf_rs, rs_ss, rs_rs, x_ss, x_rs,
    ag_ss, ag_rs, fw_ss, fw_rs, pv_ss, pv_rs,
):
    x = lax.axis_index("site")
    o = lax.axis_index("ops")
    c = o % 2
    y = (o // 2) % 4
    z = o // 8
    x_l = x + 1 - 2 * (x % 2)
    x_r = 3 - x
    to_l = {"site": x_l}
    to_r = {"site": x_r}
    sib = {"ops": o + 1 - 2 * c}
    to_ls = {"ops": o + 1 - 2 * c, "site": x_l}
    y_a = y + 1 - 2 * (y % 2)
    z_a = z + 1 - 2 * (z % 2)
    y_c = 3 - y_a
    z_c = 3 - z_a
    x_c = 3 - x_l
    dims = (
        {"ops": o + 2 * (y_a - y)},
        {"ops": o + 8 * (z_a - z)},
        {"ops": o + 2 * (3 - 2 * y)},
        {"ops": o + 8 * (3 - 2 * z)},
    )
    far = ({"ops": o + 2 * (y_c - y)}, {"ops": o + 8 * (z_c - z)}, {"site": x_c})
    bits = label_bits(y, z)
    offs = piece_offsets(bits)
    data = pl.ds(64, W)

    def raw_copies(m):
        buf = m % 2
        return (
            pltpu.make_async_copy(left_hbm.at[pl.ds(NS * m, NS)], raw.at[buf, 0], raw_sem.at[buf, 0]),
            pltpu.make_async_copy(right_hbm.at[pl.ds(NS * m, NS)], raw.at[buf, 1], raw_sem.at[buf, 1]),
        )

    for m in range(2):
        for cp in raw_copies(m):
            cp.start()
    psi_copy = pltpu.make_async_copy(psi_hbm, psi_v, psi_sem)
    psi_copy.start()

    pvr[...] = jnp.zeros_like(pvr)
    barrier = pltpu.get_barrier_semaphore()
    for who in (to_l, to_r, sib, to_ls, *dims, *far):
        pl.semaphore_signal(barrier, inc=1, device_id=who, device_id_type=MESH)

    def l_copy(ph, m, w):
        at = pl.ds(NS * m, NS)
        tiles = pl.ds(0, 2) if ph == 0 else pl.ds(2, 1)
        return pltpu.make_async_remote_copy(
            src_ref=lall.at[c if w == 0 else 1 - c, at, tiles], dst_ref=lall.at[3 + w, at, tiles],
            send_sem=l_ss.at[ph, m, w], recv_sem=l_rs.at[ph, m, w],
            device_id=to_l if w == 0 else to_ls, device_id_type=MESH)

    def ls_copy(m):
        at = pl.ds(NS * m, NS)
        return pltpu.make_async_remote_copy(
            src_ref=lall.at[1 - c, at], dst_ref=lall.at[2, at], send_sem=ls_ss.at[m], recv_sem=ls_rs.at[m],
            device_id=sib, device_id_type=MESH)

    def r_copy(p, m):
        at = pl.ds(NS * m, NS)
        return pltpu.make_async_remote_copy(
            src_ref=rb.at[0, p, at, :, data, :], dst_ref=rb.at[2, p, at, :, data, :],
            send_sem=r_ss.at[p, m], recv_sem=r_rs.at[p, m], device_id=to_r, device_id_type=MESH)

    def ro_copy(m):
        at = pl.ds(NS * m, NS)
        return pltpu.make_async_remote_copy(
            src_ref=rb.at[0, :, at, :, data, :], dst_ref=rb.at[1, :, at, :, data, :],
            send_sem=ro_ss.at[m], recv_sem=ro_rs.at[m], device_id=sib, device_id_type=MESH)

    def rf_copy(p, m):
        at = pl.ds(NS * m, NS)
        return pltpu.make_async_remote_copy(
            src_ref=rb.at[2, p, at, :, data, :], dst_ref=rb.at[3, p, at, :, data, :],
            send_sem=rf_ss.at[p, m], recv_sem=rf_rs.at[p, m], device_id=sib, device_id_type=MESH)

    def pack(m):
        buf = m % 2

        def one(k, carry):
            s = k // 2
            p = k % 2
            slot = NS * m + s
            row = iota((W, 128), 0)
            live = slot < count[0]
            keep = []
            for n in range(2):
                size = jnp.where(live, lsize[x * 4 + 2 * n + p], 0)
                keep.append(one_hot(row < size))
            ev = raw[buf, 0, s, p]
            od = raw[buf, 0, s, 2 + p]
            lall[p, slot, 0] = ev[:, :128] * keep[0]
            lall[p, slot, 2] = od[:, :128] * keep[1]
            lall[p, slot, 1] = jnp.concatenate(
                [ev[:, 128:] * keep[0][:, :64], od[:, 128:] * keep[1][:, :64]], axis=1)
            ev = raw[buf, 1, s, 2 * p]
            od = raw[buf, 1, s, 2 * p + 1]
            rb[0, p, slot, 0, data, :] = ev[:, :128]
            rb[0, p, slot, 1, data, :] = od[:, :128]
            rb[0, p, slot, 2, data, :] = jnp.concatenate([ev[:, 128:], od[:, 128:]], axis=1)
            return carry

        lax.fori_loop(0, 2 * NS, one, 0)

    for m in range(NC):
        for cp in raw_copies(m):
            cp.wait()
        pack(m)
        if m == 0:
            pl.semaphore_wait(barrier, 11)
        if m + 2 < NC:
            for cp in raw_copies(m + 2):
                cp.start()
        for w in range(2):
            l_copy(0, m, w).start()
        r_copy(0, m).start()
        ls_copy(m).start()
        ro_copy(m).start()
    for m in range(NC):
        for w in range(2):
            l_copy(1, m, w).start()
        r_copy(1, m).start()

    def piece(g, qi):
        off = offs[g][qi][-1]
        n = off // W
        l, r = cell_at(g, qi, n)
        return 2 * l + c, off - n * W, r

    def sub_copy(g, qi, k):
        i, a0, r = piece(g, qi)
        return pltpu.make_async_copy(
            sub_hbm.at[k, i, pl.ds(pl.multiple_of(a0, 16), 48), :],
            subv.at[g * 4 + qi, k], sub_sem.at[g * 4 + qi, k])

    for g in range(CHUNKS):
        for qi in range(4):
            for k in range(2):
                sub_copy(g, qi, k).start()

    zrow = jnp.zeros((SLOTS, 3, 64, 128), BF)

    def clear(k, carry):
        for start in (0, 256):
            rb[k // 2, k % 2, :, :, pl.ds(start, 64), :] = zrow
        acc[2 * k] = jnp.zeros((W, 384), F32)
        acc[2 * k + 1] = jnp.zeros((W, 384), F32)
        return carry

    lax.fori_loop(0, 8, clear, 0)

    psi_copy.wait()

    def row_hot(q, first, rows, half):
        rs = lstart[q]
        t0 = jnp.minimum(rs // 16, BOND // 16 - 16)
        pos = iota((rows, 256), 0) + first
        if half is None:
            idx, ok = pos, pos < W
        else:
            idx, ok = packed_index(pos, half)
        ok = ok & (idx < lsize[q])
        return t0, one_hot(ok & (iota((rows, 256), 1) == idx + (rs - t0 * 16)))

    def put_rows(at, rows, t0, hot):
        for n in range(4):
            win = jnp.concatenate([psi_v[t0 + k, :, pl.ds(n * 512, 512)] for k in range(16)], axis=0)
            got = jnp.dot(hot, win, preferred_element_type=F32).astype(BF)
            for k in range(4):
                gath[n * 4 + k, pl.ds(at, rows), :] = got[:, k * 128:(k + 1) * 128]

    def rows_of(i, carry):
        q = jnp.where(i < 2, x, x_l) * 4 + 2 * (i % 2) + c
        t0, hot = row_hot(q, 0, 256, i % 2)
        put_rows(pl.multiple_of(i * 256, 256), 256, t0, hot)
        return carry

    lax.fori_loop(0, 4, rows_of, 0)

    def cols_of(j, carry):
        q = jnp.where(j < 4, x * 4 + j, x_r * 4 + j - 4)
        cs = rstart[q]
        ct = jnp.minimum(cs // 128, BOND // 128 - 3)
        idx, ok = packed_index(iota((384, 256), 1), q % 2)
        ok = ok & (idx < rsize[q])
        hot = one_hot(ok & (iota((384, 256), 0) == idx + (cs - ct * 128)))
        for m in range(2):
            win = jnp.concatenate([gath[ct + k, pl.ds(m * 512, 512), :] for k in range(3)], axis=1)
            pp[j, pl.ds(m * 512, 512), :] = jnp.dot(win, hot, preferred_element_type=F32).astype(BF)
        return carry

    lax.fori_loop(0, 8, cols_of, 0)

    def own_rows():
        re = renergy[...]
        hi = re.astype(BF)
        rem = re - hi.astype(F32)
        mid = rem.astype(BF)
        low = (rem - mid.astype(F32)).astype(BF)
        rows16 = iota((16, BOND), 0)
        er3 = jnp.where(rows16 == 0, hi.astype(F32),
                        jnp.where(rows16 == 1, mid.astype(F32),
                                  jnp.where(rows16 == 2, low.astype(F32), F32(0)))).astype(BF)
        for t in range(16):
            for qi in range(4):
                gath[t, pl.ds(qi * 160 + 144, 16), :] = er3[:, t * 128:(t + 1) * 128]
        for g in range(CHUNKS):
            for qi in range(4):
                n8 = g * 4 + qi
                at = qi * 160
                i, a0, r = piece(g, qi)
                q = x * 4 + i
                t0, hot = row_hot(q, a0, 48, None)
                put_rows(at, 48, t0, hot)
                for k in range(2):
                    sub_copy(g, qi, k).wait()
                    for t in range(16):
                        gath[t, pl.ds(at + 48 + 48 * k, 48), :] = subv[n8, k, :, pl.ds(t * 128, 128)]
                xt = x if CELLS[g][qi][0] == 0 else x_l
                site = xt + (r // 2) * (3 - 2 * xt)
                total = None
                for par in range(2):
                    qr = site * 4 + 2 * (r % 2) + par
                    cs = rstart[qr]
                    ct = jnp.minimum(cs // 128, BOND // 128 - 3)
                    j = iota((384, 384), 1) - W * par
                    hot2 = one_hot((j >= 0) & (j < W) & (j < rsize[qr])
                                   & (iota((384, 384), 0) == j + (cs - ct * 128)))
                    win = jnp.concatenate([gath[ct + k, pl.ds(at, 160), :] for k in range(3)], axis=1)
                    part = jnp.dot(win, hot2, preferred_element_type=F32)
                    total = part if total is None else total + part
                lt = jnp.minimum(lstart[q] // 128, BOND // 128 - 3)
                shift = lstart[q] - lt * 128 + a0
                pick = iota((48, 384), 1) == iota((48, 384), 0) + shift
                lrow = jnp.concatenate([lenergy[lt + k] for k in range(3)], axis=1)
                el = jnp.sum(jnp.where(pick, lrow, F32(0)), axis=1, keepdims=True)
                er = total[144:145] + total[145:146] + total[146:147]
                diag[n8] = (el + er) * total[:48]
                subp[n8, 0] = total[48:96]
                subp[n8, 1] = total[96:144]

    left_at = {(0, 0): c, (0, 1): 2, (1, 0): 3, (1, 1): 4}

    def product(m, w, r, lefts):
        slots = pl.ds(NS * m, NS)
        side = (0 if r < 2 else 2) + w
        for par in range(2):
            j = 2 * r + par
            for n, (h, l) in enumerate(lefts):
                src = left_at[(h, w)]
                lhs = jnp.concatenate([lall[src, slots, 2 * l].reshape(NS * W, 128),
                                       lall[src, slots, 1].reshape(NS * W, 128)], axis=1)
                img = jnp.dot(lhs, pp[j, pl.ds((2 * h + l) * 256, 256), :],
                              preferred_element_type=F32).astype(BF)
                for s in range(NS):
                    li[pl.ds(n * W, W), pl.ds(s * 256, 256)] = img[s * W:(s + 1) * W]
            rows = pl.ds(64 - 64 * par, 256)
            rhs = jnp.concatenate(
                [rb[side, r % 2, NS * m + s, k, rows, :] for s in range(NS) for k in (par, 2)], axis=1)
            lanes = pl.ds(128 * par, 256)
            res = lax.dot_general(li[pl.ds(0, len(lefts) * W), :], rhs, (((1,), (1,)), ((), ())),
                                  preferred_element_type=F32)
            for n, (h, l) in enumerate(lefts):
                acc[PLACE[(h, l, r)], :, lanes] += res[n * W:(n + 1) * W]

    def arrive(p, m):
        r_copy(p, m).wait()
        rf_copy(p, m).start()
        for w in range(2):
            l_copy(p, m, w).wait()

    def landing(g, qi, s):
        steps = STEPS[g]
        if s == 3:
            return rs3.at[g, qi], 48, True
        if s == len(steps):
            return rs4.at[g, qi], 48, True
        rows = steps[s]
        return {192: rs0.at[qi], 96: rs1.at[g, qi], 48: rs2.at[g, qi]}[rows], rows, False

    def lanes_of(g, pt, first=0):
        start, width = PARTS[g][pt]
        return pl.ds(pl.multiple_of(first + start, 128), width)

    def strip(g, qi, first, rows):
        n = first // W
        return BASE[g] + qi * len(CELLS[g][qi][1]) + n, pl.ds(pl.multiple_of(first - n * W, 16), rows)

    def rs_copy(g, qi, s, pt):
        d = (qi + s) % 4
        dst, rows, whole = landing(g, qi, s)
        first = offs[g][qi][-1] if whole else offs[g][qi][s] + (1 - bits[d]) * rows
        n, at = strip(g, qi, first, rows)
        return pltpu.make_async_remote_copy(
            src_ref=acc.at[n, at, lanes_of(g, pt)], dst_ref=dst.at[:, lanes_of(g, pt)],
            send_sem=rs_ss.at[g, qi, s, pt], recv_sem=rs_rs.at[g, qi, s, pt],
            device_id=dims[d], device_id_type=MESH)

    def add_rows(g, qi, first, src, rows, pt):
        lanes = lanes_of(g, pt)
        n = first // W
        row = first - n * W
        n = BASE[g] + qi * len(CELLS[g][qi][1]) + n

        def step(k, carry):
            at = pl.ds(pl.multiple_of(row + k * 48, 16), 48)
            acc[n, at, lanes] += src[pl.ds(pl.multiple_of(k * 48, 16), 48), lanes]
            return carry

        lax.fori_loop(0, rows // 48, step, 0)

    def x_copy(g, qi, pt):
        lanes = lanes_of(g, pt)
        n, at = strip(g, qi, offs[g][qi][-1], 48)
        return pltpu.make_async_remote_copy(
            src_ref=acc.at[n, at, lanes], dst_ref=xrecv.at[g, qi, :, lanes],
            send_sem=x_ss.at[g, qi, pt], recv_sem=x_rs.at[g, qi, pt], device_id=to_l, device_id_type=MESH)

    def reduce_step(g, s, pt=0):
        for qi in range(4):
            src, rows, whole = landing(g, qi, s)
            rs_copy(g, qi, s, pt).wait_recv()
            if whole:
                rs_copy(g, qi, s, pt).wait_send()
            add_rows(g, qi, offs[g][qi][-1] if whole else offs[g][qi][s + 1], src, rows, pt)
            if s < 3:
                rs_copy(g, qi, s + 1, pt).start()
            elif CELLS[g][qi][0] == 1:
                x_copy(g, qi, pt).start()

    def rows_at(g, qi, first, rows, core, pt):
        n = first // W
        l, r = cell_at(g, qi, n)
        tile = CELLS[g][qi][0] * 48 + (2 * l + core) * 12 + (first - n * W) // 16
        return pl.ds(tile, rows // 16), lanes_of(g, pt, r * 384)

    def ag_copy(g, qi, s, mine, pt):
        d = (qi + s) % 4
        rows = STEPS[g][s]
        first = offs[g][qi][s + 1] if mine else offs[g][qi][s] + (1 - bits[d]) * rows
        at, lanes = rows_at(g, qi, first, rows, c, pt)
        return pltpu.make_async_remote_copy(
            src_ref=psi_v.at[at, :, lanes], dst_ref=psi_v.at[at, :, lanes],
            send_sem=ag_ss.at[g, qi, s, pt], recv_sem=ag_rs.at[g, qi, s, pt],
            device_id=dims[d], device_id_type=MESH)

    def fw_copy(g, qi, s, core, pt):
        if s == 3:
            first, rows = offs[g][qi][-1], 48
        else:
            rows = STEPS[g][s]
            first = offs[g][qi][s] + (1 - bits[(qi + s) % 4]) * rows
        at, lanes = rows_at(g, qi, first, rows, core, pt)
        return pltpu.make_async_remote_copy(
            src_ref=psi_v.at[at, :, lanes], dst_ref=psi_v.at[at, :, lanes],
            send_sem=fw_ss.at[g, qi, s, pt], recv_sem=fw_rs.at[g, qi, s, pt],
            device_id=sib, device_id_type=MESH)

    totals = [jnp.zeros((48, 128), F32), jnp.zeros((48, 128), F32)]

    def finish(g, h, pt=0):
        lanes = lanes_of(g, pt)
        for qi in range(4):
            if CELLS[g][qi][0] != h:
                continue
            off = offs[g][qi][-1]
            if h == 0:
                n, rows = strip(g, qi, off, 48)
                part = acc[n, rows, lanes]
            else:
                x_copy(g, qi, pt).wait_recv()
                part = xrecv[g, qi, :, lanes]
            full = part + diag[g * 4 + qi, :, lanes]
            at, where = rows_at(g, qi, off, 48, c, pt)
            width = PARTS[g][pt][1]
            psi_v[at, :, where] = full.astype(BF).reshape(3, 16, width)
            ag_copy(g, qi, len(STEPS[g]) - 1, True, pt).start()
            fw_copy(g, qi, 3, c, pt).start()
            weight = 1 - bits[(qi + 3) % 4]
            if len(STEPS[g]) == 2:
                weight = weight * (1 - bits[(qi + 2) % 4])
            weight = weight.astype(F32)
            for k in range(2):
                prod = weight * full * subp[g * 4 + qi, k, :, lanes]
                for t in range(width // 128):
                    totals[k] = totals[k] + prod[:, t * 128:(t + 1) * 128]

    def gather_step(g, s, pt=0):
        for qi in range(4):
            ag_copy(g, qi, s, False, pt).wait_recv()
            if s > 0:
                ag_copy(g, qi, s - 1, True, pt).start()
            fw_copy(g, qi, s, c, pt).start()

    def step0(m, carry):
        for w in range(2):
            if w == 1:
                ls_copy(m).wait_recv()
                ro_copy(m).wait_recv()
            for r in range(2):
                product(m, w, r, ((0, 0), (0, 1)))
        return carry

    lax.fori_loop(0, NC, step0, 0)
    for qi in range(4):
        rs_copy(0, qi, 0, 0).start()
    own_rows()
    reduce_step(0, 0)

    def step1(m, carry):
        arrive(0, m)
        for w in range(2):
            if w == 1:
                rf_copy(0, m).wait_recv()
            for r in range(2):
                product(m, w, r, ((1, 0),))
            product(m, w, 2, ((0, 0), (0, 1), (1, 0)))
        return carry

    lax.fori_loop(0, NC // 2, step1, 0)
    reduce_step(0, 1)
    lax.fori_loop(NC // 2, NC, step1, 0)
    for qi in range(4):
        rs_copy(1, qi, 0, 0).start()
    reduce_step(0, 2)

    def first_half(m):
        arrive(1, m)
        for w in range(2):
            for r in range(3):
                product(m, w, r, ((1, 1),))

    def second_half(m):
        for w in range(2):
            if w == 1:
                rf_copy(1, m).wait_recv()
            product(m, w, 3, ((0, 0), (0, 1), (1, 0), (1, 1)))

    first_half(0)
    reduce_step(0, 3)
    finish(0, 0)
    second_half(0)
    reduce_step(1, 0)
    gather_step(0, 1)
    first_half(1)
    second_half(1)
    reduce_step(1, 1)
    gather_step(0, 0)
    first_half(2)
    second_half(2)
    reduce_step(1, 2)
    first_half(3)
    for qi in (1, 2):
        for pt in range(2):
            rs_copy(2, qi, 0, pt).start()
    second_half(3)
    for qi in (0, 3):
        for pt in range(2):
            rs_copy(2, qi, 0, pt).start()
    reduce_step(1, 3)
    finish(1, 0)
    reduce_step(2, 0, 0)
    finish(1, 1)
    reduce_step(2, 0, 1)
    reduce_step(2, 1, 0)
    gather_step(1, 1)
    reduce_step(2, 1, 1)
    reduce_step(2, 2, 0)
    gather_step(1, 0)
    reduce_step(2, 2, 1)
    for pt in range(2):
        reduce_step(2, 3, pt)
    for pt in range(2):
        finish(2, 0, pt)
        finish(2, 1, pt)

    lane = iota((8, 128), 1)
    sums = [jnp.sum(total, keepdims=True) for total in totals]
    pvs[0] = jnp.where(lane == 0, sums[0], jnp.where(lane == 1, sums[1], F32(0)))
    rounds = (
        (c, ((sib, 1 - c),)),
        (y, ((dims[0], y_a), (dims[2], 3 - y), (far[0], y_c))),
        (z, ((dims[1], z_a), (dims[3], 3 - z), (far[1], z_c))),
        (x, ((to_l, x_l), (to_r, x_r), (far[2], x_c))),
    )

    def pv_copy(n, i, slot):
        return pltpu.make_async_remote_copy(
            src_ref=pvs.at[n], dst_ref=pvr.at[n, slot], send_sem=pv_ss.at[n, i], recv_sem=pv_rs.at[n, slot],
            device_id=rounds[n][1][i][0], device_id_type=MESH)

    def pv_send(n):
        me, others = rounds[n]
        for i in range(len(others)):
            pv_copy(n, i, me).start()
        pvr[n, me] = pvs[n]

    def pv_sum(n):
        me, others = rounds[n]
        for i, (who, slot) in enumerate(others):
            pv_copy(n, i, slot).wait_recv()
        pvs[n + 1] = (pvr[n, 0] + pvr[n, 1]) + (pvr[n, 2] + pvr[n, 3])

    def o_copy(k, core):
        return [pltpu.make_async_copy(
            psi_v.at[pl.ds((k // 4) * 48 + (2 * l + core) * 12, 12), :, pl.ds((k % 4) * 384, 384)],
            out_hbm.at[k, pl.ds((2 * l + core) * 12, 12)], out_sem.at[k, core, l]) for l in range(2)]

    pv_send(0)
    for n, s in enumerate((2, 1, 0)):
        for pt in range(2):
            gather_step(2, s, pt)
        pv_sum(n)
        pv_send(n + 1)
    for k in range(8):
        for cp in o_copy(k, c):
            cp.start()
    for g in range(CHUNKS):
        for s in (3, *reversed(range(len(STEPS[g])))):
            for qi in range(4):
                for pt in range(len(PARTS[g])):
                    fw_copy(g, qi, s, 1 - c, pt).wait_recv()
    for k in range(8):
        for cp in o_copy(k, 1 - c):
            cp.start()
    pv_sum(3)
    proj_out[...] = pvs[4]
    for g in range(CHUNKS):
        for qi in range(4):
            for pt in range(len(PARTS[g])):
                for s in range(len(STEPS[g])):
                    rs_copy(g, qi, s, pt).wait_send()
                    ag_copy(g, qi, s, True, pt).wait_send()
                    fw_copy(g, qi, s, c, pt).wait_send()
                fw_copy(g, qi, 3, c, pt).wait_send()
                if CELLS[g][qi][0] == 1:
                    x_copy(g, qi, pt).wait_send()
    for m in range(NC):
        ls_copy(m).wait_send()
        ro_copy(m).wait_send()
        for p in range(2):
            rf_copy(p, m).wait_send()
    for n in range(4):
        for i in range(len(rounds[n][1])):
            pv_copy(n, i, rounds[n][0]).wait_send()
    for k in range(8):
        for core in (c, 1 - c):
            for cp in o_copy(k, core):
                cp.wait()


def compact_body(rstart, rsize, proj, src, out, proj_out):
    x = lax.axis_index("site")
    step = pl.program_id(0)
    x_l = x + 1 - 2 * (x % 2)

    @pl.when(step == 0)
    def _():
        out[...] = jnp.zeros_like(out)
        for i in range(2):
            proj_out[i] = proj[0, i]

    for n in range(4):
        k = step * 4 + n
        xt = jnp.where(k // 4 == 0, x, x_l)
        site = xt + ((k // 2) % 2) * (3 - 2 * xt)
        q = site * 4 + 2 * (k % 2)
        start = rstart[q]
        base = pl.multiple_of(jnp.minimum((start // 128) * 128, BOND - 512), 128)
        j = iota((384, 1), 0)
        odd = j >= W
        idx = jnp.where(odd, j - W, j)
        size = jnp.where(odd, rsize[q + 1], rsize[q])
        first = jnp.where(odd, rstart[q + 1], start) - base
        target = jnp.where(idx < size, idx + first, -1)
        hot = one_hot(iota((384, 512), 1) == target)
        out[:, pl.ds(base, 512)] += jnp.dot(src[n], hot, preferred_element_type=F32).astype(BF)


def sector_tables(sector_ids, sectors):
    labels = jnp.arange(sectors, dtype=jnp.int32)
    starts = jnp.sum((sector_ids[None, :] < labels[:, None]).astype(jnp.int32), axis=1)
    sizes = jnp.sum((sector_ids[None, :] == labels[:, None]).astype(jnp.int32), axis=1)
    return starts, sizes


def local(wavefunction, left_blocks, right_blocks, left_sector, right_sector, term_count,
          left_energy, right_energy, subspace):
    lstart, lsize = sector_tables(left_sector, 16)
    rstart, rsize = sector_tables(right_sector, 16)
    smem = pl.BlockSpec(memory_space=pltpu.SMEM)
    vmem = pl.BlockSpec(memory_space=pltpu.VMEM)
    hbm = pl.BlockSpec(memory_space=pl.ANY)
    dma = pltpu.SemaphoreType.DMA
    slabs, proj = pl.pallas_call(
        body,
        out_shape=(jax.ShapeDtypeStruct((8, 48, 16, 384), BF), jax.ShapeDtypeStruct((8, 128), F32)),
        in_specs=[smem] * 5 + [hbm] * 3 + [vmem] * 2 + [hbm],
        out_specs=(hbm, vmem),
        scratch_shapes=[
            pltpu.VMEM((BOND // 16, 16, BOND), BF),
            pltpu.VMEM((16, 1024, 128), BF),
            pltpu.VMEM((8, 1024, 256), BF),
            pltpu.VMEM((2, 2, NS, 4, W, W), BF),
            pltpu.VMEM((5, SLOTS, 3, W, 128), BF),
            pltpu.VMEM((4, 2, SLOTS, 3, 320, 128), BF),
            pltpu.VMEM((768, NS * 256), BF),
            pltpu.VMEM((16, W, 384), F32),
            pltpu.VMEM((12, 2, 48, BOND), BF),
            pltpu.VMEM((12, 48, 384), F32),
            pltpu.VMEM((12, 2, 48, 384), F32),
            pltpu.VMEM((4, 192, 384), F32),
            pltpu.VMEM((3, 4, 96, 384), F32),
            pltpu.VMEM((3, 4, 48, 384), F32),
            pltpu.VMEM((3, 4, 48, 384), F32),
            pltpu.VMEM((2, 4, 48, 384), F32),
            pltpu.VMEM((3, 4, 48, 384), F32),
            pltpu.VMEM((5, 8, 128), F32),
            pltpu.VMEM((4, 4, 8, 128), F32),
            dma((2, 2)), dma, dma((12, 2)), dma((8, 2, 2)),
            dma((2, NC, 2)), dma((2, NC, 2)), dma((NC,)), dma((NC,)), dma((2, NC)), dma((2, NC)),
            dma((NC,)), dma((NC,)), dma((2, NC)), dma((2, NC)),
            dma((3, 4, 4, 2)), dma((3, 4, 4, 2)), dma((3, 4, 2)), dma((3, 4, 2)),
            dma((3, 4, 3, 2)), dma((3, 4, 3, 2)), dma((3, 4, 4, 2)), dma((3, 4, 4, 2)), dma((4, 3)), dma((4, 4)),
        ],
        compiler_params=pltpu.CompilerParams(
            collective_id=0, has_side_effects=True, vmem_limit_bytes=67043328),
        name="exchange",
    )(lstart, lsize, rstart, rsize, term_count, wavefunction.reshape(BOND // 16, 16, BOND),
      left_blocks, right_blocks, left_energy.reshape(16, 1, 128), right_energy.reshape(1, BOND), subspace)
    sigma, projections = pl.pallas_call(
        compact_body,
        grid=(2,),
        out_shape=(jax.ShapeDtypeStruct((768, BOND), BF), jax.ShapeDtypeStruct((2,), F32)),
        in_specs=[smem, smem, smem, pl.BlockSpec((4, 768, 384), lambda k: (k, 0, 0))],
        out_specs=(pl.BlockSpec((768, BOND), lambda k: (0, 0)), smem),
        name="compact",
    )(rstart, rsize, proj, slabs.reshape(8, 768, 384))
    return sigma.reshape(4, W, BOND), projections


def solution(mesh):
    in_specs = (P(), P("ops", "site", None, None), P("ops", "site", None, None), P(), P(), P("ops"),
                P(), P(), P(None, "site", None, None))
    out_specs = (P("site", None, None), P())
    return jax.shard_map(local, mesh=mesh, in_specs=in_specs, out_specs=out_specs, check_vma=False)
```
